32 devices in a mesh: region: 2 (over x), blk: 16 (over z, y, core).
Axes of the slice: x: 2, y: 2, z: 4, core: 2. Of those that a mesh axis runs over, the one named last changes fastest.
Arguments:
- ensemble: float32 [64, 256, 128], P(('region', 'blk'))
- observed: float32 [64, 256, 128], P(('region', 'blk')), may hold values from -6 to 6
- obs_var: float32 [64, 256], P(('region', 'blk')), may hold values from 0.5 to 2
- ridge: float32 [64], P(('region', 'blk')), may hold values from 0.05 to 0.5
- pred_back: int32 [64, 12], P(('region', 'blk')), may hold values from 0 to 16, as said below
- bounds: float32 [2], replicated, may hold values from 0.2 to 6, as said below
Outputs:
- analysis: float32 [64, 256, 128], P(('region', 'blk'))
The draws below stay inside these ranges and needn't reach their ends.
Inputs may be any that keep to these rules, and one draw needn't show every extreme that they name: `pred_back`: each row holds distinct distances among 1 to 16, never more than the block's own index, with 0 for an empty slot; the last block fills all 12 slots. bounds[0] < bounds[1].
All inputs are finite; a program needn't handle non-finite values.
Results may differ from the reference program's by a relative error of at most 0.0003.
Values sent between devices are 32-bit elements; how exact they have to be, the bound alone decides.
A program may use at most 192 MiB of HBM per device.

```python
import math
import jax
import jax.numpy as jnp
from jax import lax

M = 128
ROWS = 256
SLOTS = 12
REACH = 16
ITERS = 3
NBLK = 64


def draw_ensemble(key, part):
    first = jax.random.fold_in(jax.random.fold_in(key, 11), 0)
    noise = jax.random.normal(first, (NBLK, ROWS, M), jnp.float32)

    def advance(carry, fresh):
        state = 0.8 * carry + 0.6 * fresh
        return (state, state)
    start = jnp.zeros((ROWS, M), jnp.float32)
    unused, analysis_output = lax.scan(advance, start, noise)
    return analysis_output


def draw_pred_back(key, part):
    first, second, third = jax.random.split(jax.random.fold_in(key, 23), 3)
    scores = jax.random.randint(first, (NBLK, REACH), 0, 1 << 20) * REACH + jnp.arange(REACH, dtype=jnp.int32)[None, :]
    order = jnp.argsort(scores, axis=1).astype(jnp.int32)
    distance = order[:, :SLOTS] + 1
    base = jax.random.randint(second, (NBLK,), 1, 8)
    many = jax.random.randint(third, (NBLK,), 0, 8) == 0
    blocks = jnp.arange(NBLK, dtype=jnp.int32)
    count = jnp.where(many | (blocks == NBLK - 1), SLOTS, base)
    slot_index = jnp.arange(SLOTS, dtype=jnp.int32)
    chosen = jnp.where(slot_index[None, :] < count[:, None], distance, 0)
    chosen = jnp.where(chosen <= blocks[:, None], chosen, 0)
    return chosen.astype(jnp.int32)


def draw_bounds(key, part):
    first, second = jax.random.split(jax.random.fold_in(key, 37))
    lower_bound = jax.random.uniform(first, (1,), jnp.float32, 0.2, 0.5)
    upper_bound = jax.random.uniform(second, (1,), jnp.float32, 3.0, 6.0)
    return jnp.concatenate([lower_bound, upper_bound])


def shard_levels(stream_key, dims, cuts, smallest, largest):
    gain = 1.0
    for axis_at, parts in cuts:
        heights = jax.random.uniform(jax.random.fold_in(jax.random.fold_in(stream_key, 6), axis_at), (parts,), jnp.float32, smallest / len(cuts), largest / len(cuts))
        gain = gain * jnp.repeat(jnp.exp(heights), dims[axis_at] // parts).reshape((-1,) + (1,) * (len(dims) - 1 - axis_at))
    return gain


def normal_values(rng, extent, spread, bound, cuts=(), held_as=jnp.bfloat16):
    result = spread * jax.random.normal(rng, extent, jnp.float32)
    if cuts:
        result = result * shard_levels(rng, extent, cuts, -0.22, 0.18)
    return jnp.clip(result, -bound, bound).astype(held_as)


def setup_inputs(seed: int = 0) -> dict:
    arg_keys = jax.random.split(jax.random.key(seed), 7)
    ensemble = draw_ensemble(jax.random.fold_in(arg_keys[6], 71), 0)
    observed = normal_values(arg_keys[1], (NBLK, ROWS, M), 1.0, 6.0, ((0, 32),), jnp.float32)
    obs_var = jnp.clip(jnp.exp(math.log(2.0) - 1.3862944 * jax.random.uniform(arg_keys[2], (NBLK, ROWS), jnp.float32) ** shard_levels(arg_keys[2], (NBLK, ROWS), ((0, 32),), -0.2, 0.2)), 0.5, 2.0)
    ridge = jnp.clip(jnp.exp(math.log(0.5) - 2.3025851 * jax.random.uniform(arg_keys[3], (NBLK,), jnp.float32) ** shard_levels(arg_keys[3], (NBLK,), ((0, 32),), -0.2, 0.2)), 0.05, 0.5)
    pred_back = draw_pred_back(jax.random.fold_in(arg_keys[6], 71), 0)
    bounds = draw_bounds(jax.random.fold_in(arg_keys[6], 71), 0)
    return {"ensemble": ensemble, "observed": observed, "obs_var": obs_var, "ridge": ridge, "pred_back": pred_back, "bounds": bounds}


def small_solve(gram, target):
    size = gram.shape[0]
    factor = {}
    for block_position in range(size):
        running = gram[block_position, block_position]
        for k in range(block_position):
            running = running - factor[block_position, k] * factor[block_position, k]
        factor[block_position, block_position] = jnp.sqrt(running)
        for i in range(block_position + 1, size):
            running = gram[i, block_position]
            for k in range(block_position):
                running = running - factor[i, k] * factor[block_position, k]
            factor[i, block_position] = running / factor[block_position, block_position]
    forward = []
    for i in range(size):
        running = target[i]
        for k in range(i):
            running = running - factor[i, k] * forward[k]
        forward.append(running / factor[i, i])
    analysis_output = [None] * size
    for i in reversed(range(size)):
        running = forward[i]
        for k in range(i + 1, size):
            running = running - factor[k, i] * analysis_output[k]
        analysis_output[i] = running / factor[i, i]
    return jnp.stack(analysis_output)

def reference(ensemble, observed, obs_var, ridge, pred_back, bounds):
    highest = lax.Precision.HIGHEST
    nblocks = ensemble.shape[0]
    members = ensemble.shape[2]
    slots = pred_back.shape[1]
    anomaly = (ensemble - lax.optimization_barrier(jnp.mean(ensemble, axis=2, keepdims=True))) / jnp.sqrt(jnp.float32(members - 1))
    empty_zero_matrix = jnp.zeros((1,) + ensemble.shape[1:], ensemble.dtype)
    padded = jnp.concatenate([anomaly, empty_zero_matrix], axis=0)
    block_index_list = jnp.arange(nblocks, dtype=jnp.int32)[:, None] - pred_back
    block_index_list = jnp.where(pred_back > 0, block_index_list, nblocks).astype(jnp.int32)
    identity = jnp.eye(slots, dtype=jnp.float32)

    def regress(inputs):
        own, picked, weight = inputs
        preds = padded[picked]
        gram = jnp.einsum('jrm,krm->jkr', preds, preds, precision=highest) + weight * identity[:, :, None]
        target = jnp.einsum('jrm,rm->jr', preds, own, precision=highest)
        regression_coefficients = small_solve(gram, target)
        resid = own - jnp.einsum('jr,jrm->rm', regression_coefficients, preds, precision=highest)
        return (regression_coefficients, lax.optimization_barrier(jnp.sum(resid * resid, axis=1)) + 1e-05)
    regression_coefficients, dvar = lax.map(regress, (anomaly, block_index_list, ridge))

    def lower(entry_values):
        padded_entry_values = jnp.concatenate([entry_values, empty_zero_matrix], axis=0)
        analysis_output = entry_values
        for block_position in range(slots):
            analysis_output = analysis_output - regression_coefficients[:, block_position, :, None] * padded_entry_values[block_index_list[:, block_position]]
        return analysis_output

    def upper(entry_values):
        analysis_output = jnp.concatenate([entry_values, empty_zero_matrix], axis=0)
        for block_position in range(slots):
            analysis_output = analysis_output.at[block_index_list[:, block_position]].add(-regression_coefficients[:, block_position, :, None] * entry_values)
        return analysis_output[:nblocks]
    inverse_obs = 1.0 / obs_var

    def operator(entry_values):
        return upper(lower(entry_values) / dvar[:, :, None]) + inverse_obs[:, :, None] * entry_values
    lower_bound = bounds[0]
    upper_bound = bounds[1]
    theta = (upper_bound + lower_bound) / 2
    delta = (upper_bound - lower_bound) / 2
    sigma = theta / delta
    rho_now = 1.0 / sigma
    residue = inverse_obs[:, :, None] * (observed - ensemble)
    increment = jnp.zeros_like(ensemble)
    direction = residue / theta
    for step in range(ITERS):
        increment = increment + direction
        residue = residue - operator(direction)
        rho_next = 1.0 / (2 * sigma - rho_now)
        direction = rho_next * rho_now * direction + 2 * rho_next / delta * residue
        rho_now = rho_next
    increment = increment + direction
    return ensemble + increment
```

```python
import functools
import math

import jax
import jax.numpy as jnp
from jax import lax
from jax.experimental import pallas as pl
from jax.experimental.pallas import tpu as pltpu
from jax.sharding import PartitionSpec as P

REACH = 16
ITERS = 3


def from_behind(value, axis, steps):
    count = lax.axis_size(axis)
    first, last = (max(0, -steps), min(count, count - steps))
    return lax.ppermute(value, axis, [(source, source + steps) for source in range(first, last)])


def small_solve(gram, target):
    size = gram.shape[0]
    factor = {}
    for block_position in range(size):
        running = gram[block_position, block_position]
        for k in range(block_position):
            running = running - factor[block_position, k] * factor[block_position, k]
        factor[block_position, block_position] = jnp.sqrt(running)
        for i in range(block_position + 1, size):
            running = gram[i, block_position]
            for k in range(block_position):
                running = running - factor[i, k] * factor[block_position, k]
            factor[i, block_position] = running / factor[block_position, block_position]
    forward = []
    for i in range(size):
        running = target[i]
        for k in range(i):
            running = running - factor[i, k] * forward[k]
        forward.append(running / factor[i, i])
    analysis_output = [None] * size
    for i in reversed(range(size)):
        running = forward[i]
        for k in range(i + 1, size):
            running = running - factor[k, i] * analysis_output[k]
        analysis_output[i] = running / factor[i, i]
    return jnp.stack(analysis_output)


def previous_blocks(entry_values, reach_devices):
    pieces = [
        from_behind(entry_values, ("region", "blk"), shift_by)
        for shift_by in range(reach_devices, 0, -1)
    ]
    return jnp.concatenate(pieces, axis=0)


def on_device(ensemble, observed, obs_var, ridge, pred_back, bounds):
    highest = lax.Precision.HIGHEST
    local_blocks, rows, members = ensemble.shape
    slots = pred_back.shape[1]
    reach_devices = -(-REACH // local_blocks)
    before = reach_devices * local_blocks
    anomaly = (ensemble - jnp.mean(ensemble, axis=2, keepdims=True)) / jnp.sqrt(
        jnp.float32(members - 1)
    )
    positions = before + jnp.arange(local_blocks, dtype=jnp.int32)[:, None] - pred_back
    positions = jnp.where(pred_back > 0, positions, before + local_blocks)
    empty_zero_matrix = jnp.zeros((1, rows, members), jnp.float32)

    def extend(entry_values):
        return jnp.concatenate(
            [previous_blocks(entry_values, reach_devices), entry_values, empty_zero_matrix], axis=0
        )

    preds = extend(anomaly)[positions]
    identity = jnp.eye(slots, dtype=jnp.float32)
    gram = jnp.einsum("bjrm,bkrm->jkbr", preds, preds, precision=highest)
    gram = gram + ridge[None, None, :, None] * identity[:, :, None, None]
    target = jnp.einsum("bjrm,brm->jbr", preds, anomaly, precision=highest)
    regression_coefficients = small_solve(gram, target)
    resid = anomaly - jnp.einsum("jbr,bjrm->brm", regression_coefficients, preds, precision=highest)
    inverse_var = 1.0 / (jnp.sum(resid * resid, axis=2) + 1e-05)
    inverse_obs = 1.0 / obs_var
    beta_blocks = jnp.transpose(regression_coefficients, (1, 0, 2))
    lower_bound = bounds[0]
    upper_bound = bounds[1]
    theta = (upper_bound + lower_bound) / 2
    delta = (upper_bound - lower_bound) / 2
    sigma = theta / delta
    rho_now = 1.0 / sigma
    residue = inverse_obs[:, :, None] * (observed - ensemble)
    increment = jnp.zeros_like(ensemble)
    direction = residue / theta
    for step in range(ITERS):
        increment = increment + direction
        extended = extend(direction)
        lower_analysis_output = direction
        for lower_slot in range(slots):
            lower_analysis_output = (
                lower_analysis_output
                - beta_blocks[:, lower_slot, :, None] * extended[positions[:, lower_slot]]
            )
        upper_entry_values = lower_analysis_output * inverse_var[:, :, None]
        window = jnp.zeros((before + local_blocks + 1, rows, members), jnp.float32)
        for slot in range(slots):
            window = window.at[positions[:, slot]].add(
                beta_blocks[:, slot, :, None] * upper_entry_values
            )
        analysis_output = upper_entry_values - window[before : before + local_blocks]
        for shift_by in range(1, reach_devices + 1):
            start = (reach_devices - shift_by) * local_blocks
            analysis_output = analysis_output - from_behind(
                window[start : start + local_blocks], ("region", "blk"), -shift_by
            )
        residue = residue - (analysis_output + inverse_obs[:, :, None] * direction)
        rho_next = 1.0 / (2 * sigma - rho_now)
        direction = rho_next * rho_now * direction + 2 * rho_next / delta * residue
        rho_now = rho_next
    increment = increment + direction
    return ensemble + increment


VMEM_GRANT = 66_700_000
SUB = 8
HALF = SUB // 2
LANES = 128
MESH_ID = pl.DeviceIdType.MESH
HIGHEST = lax.Precision.HIGHEST


def place():
    per = lax.axis_size("blk")
    region, blk = lax.axis_index("region"), lax.axis_index("blk")
    return lax.axis_size("region"), per, region, blk, region * per + blk


def each_peer(where, visit):
    regions, per, region, blk, unused = where
    half = per // 2
    mine = blk // half

    def on(base):
        def step(i, carry):
            to = lax.rem(region + lax.rem(i, regions), regions)
            at = base + lax.rem(blk + i // regions, half)
            visit((to, at), to * per + at)
            return carry

        return step

    lax.fori_loop(0, regions * half, on((1 - mine) * half), 0)
    lax.fori_loop(1, regions * half, on(mine * half), 0)


def copy_to(src, dst, send_sem, recv_sem, device):
    return pltpu.make_async_remote_copy(
        src_ref=src,
        dst_ref=dst,
        send_sem=send_sem,
        recv_sem=recv_sem,
        device_id=device,
        device_id_type=MESH_ID,
    )


def tile_at(k):
    return pl.ds(pl.multiple_of(k * SUB, SUB), SUB)


def swap(x):
    return pltpu.roll(x, HALF, 0)


def pair_rows(n, src, dst):
    low = lax.broadcasted_iota(jnp.int32, (SUB, LANES), 0) < HALF
    for k in range(n):
        at = slice(k * SUB, (k + 1) * SUB)
        first, second = src[0, at, :], src[1, at, :]
        dst[0, at, :] = jnp.where(low, first, swap(second))
        dst[1, at, :] = jnp.where(low, swap(first), second)


def fill_pack(rows, obs_var, ridge, pred_back, pack):
    local = pred_back.shape[0]
    lane = lax.broadcasted_iota(jnp.int32, (1, LANES), 1)
    groups = LANES // SUB
    for block in range(local):
        meta = jnp.where(lane == SUB + REACH, ridge[block], 0.0)
        for slot in range(pred_back.shape[1]):
            back = pred_back[block, slot]
            meta = jnp.where((lane == back + (SUB - 1)) & (lane >= SUB), 1.0, meta)
        for part in range(rows // LANES):
            row = obs_var[block : block + 1, part * LANES : (part + 1) * LANES]
            for k in range(groups):
                turned = row if k == 0 else pltpu.roll(row, LANES - SUB * k, 1)
                pack[part * groups + k, block] = jnp.where(lane < SUB, turned, meta)


def whole_kernel(
    n, bounds_in, ens_in, obs_in, obs_var_in, ridge_in, pred_back_in, z,
    bounds, ens, obs, obs_var, ridge, pred_back, load_sem,
    pack, ens_s, obs_s, ens_r, obs_r, pack_r, z_s, z_r, send_sem, recv_sem,
    anom, corr, filt,
):
    where = place()
    me = where[-1]
    local, rows, members = ens.shape
    loads = [
        pltpu.make_async_copy(src, dst, load_sem.at[i])
        for i, (src, dst) in enumerate(
            (
                (ens_in, ens),
                (obs_in, obs),
                (obs_var_in, obs_var),
                (ridge_in, ridge),
                (pred_back_in, pred_back),
                (bounds_in, bounds),
            )
        )
    ]
    for load in loads:
        load.start()
    barrier = pltpu.get_barrier_semaphore()

    def signal(device, k):
        pl.semaphore_signal(barrier, inc=1, device_id=device, device_id_type=MESH_ID)

    each_peer(where, signal)
    for load in loads:
        load.wait()
    own = tile_at(me)
    pair_rows(n, ens, ens_s)
    pair_rows(n, obs, obs_s)
    fill_pack(rows, obs_var, ridge, pred_back, pack)
    mine = pl.ds(me * local, local)
    ens_r[:, own, :] = ens_s[:, own, :]
    obs_r[:, own, :] = obs_s[:, own, :]
    pack_r[mine] = pack[me]
    pl.semaphore_wait(barrier, n - 1)

    def send_ens(device, k):
        copy_to(
            ens_s.at[:, tile_at(k), :], ens_r.at[:, own, :], send_sem.at[0], recv_sem.at[0], device
        ).start()

    def send_pack(device, k):
        copy_to(pack.at[k], pack_r.at[mine], send_sem.at[1], recv_sem.at[1], device).start()

    def send_half(src, dst, h, which):
        def send(device, k):
            copy_to(
                src.at[h, tile_at(k), :], dst.at[h, own, :], send_sem.at[which], recv_sem.at[which],
                device,
            ).start()

        return send

    each_peer(where, send_ens)
    each_peer(where, send_pack)
    each_peer(where, send_half(obs_s, obs_r, 0, 2))
    each_peer(where, send_half(obs_s, obs_r, 1, 3))

    others = pl.ds(0, (n - 1) * SUB)
    whole = (
        ens_r.at[:, others, :],
        pack_r.at[pl.ds(0, (n - 1) * local)],
        obs_r.at[0, others, :],
        obs_r.at[1, others, :],
        z_r.at[0, others, :],
        z_r.at[1, others, :],
    )
    regions, per, region, blk, unused = where
    neighbour = (lax.rem(region + 1, regions), blk)

    def arrived(which):
        ref = whole[which]
        copy_to(ref, ref, send_sem.at[which], recv_sem.at[which], neighbour).wait_recv()

    arrived(0)
    make_filters(n * local, arrived, bounds, ens_r, pack_r, anom, corr, filt)
    nb = n * local
    empty = jnp.zeros((LANES - nb, members), jnp.float32)
    for h in range(2):
        arrived(2 + h)
        for r in range(HALF):
            at = pl.ds(r, nb, stride=HALF)
            gap = obs_r[h, at, :] - ens_r[h, at, :]
            gap = jnp.concatenate([gap, empty] if h == 0 else [empty, gap], axis=0)
            z_s[h, at, :] = dot(filt[r, h * nb : (h + 1) * nb, :], gap, 1, 0)
        each_peer(where, send_half(z_s, z_r, h, 4 + h))
        z_r[h, own, :] = z_s[h, own, :]
    low = lax.broadcasted_iota(jnp.int32, (SUB, LANES), 0) < HALF
    arrived(4)
    arrived(5)
    for k in range(n):
        at = slice(k * SUB, (k + 1) * SUB)
        first, second = z_r[0, at, :], z_r[1, at, :]
        z[0, at, :] = jnp.where(low, first, swap(second))
        z[1, at, :] = jnp.where(low, swap(first), second)
    for which, ref in enumerate(whole):
        copy_to(ref, ref, send_sem.at[which], recv_sem.at[which], neighbour).wait_send()


def dot(lhs, rhs, left, right):
    return lax.dot_general(
        lhs,
        rhs,
        (((left,), (right,)), ((), ())),
        precision=HIGHEST,
        preferred_element_type=jnp.float32,
    )


def make_filters(nb, arrived, bounds, ens, pack, anom, corr, filt):
    members = ens.shape[2]
    square = (LANES, LANES)
    tile = (SUB, LANES)
    back = lax.broadcasted_iota(jnp.int32, square, 1) - lax.broadcasted_iota(jnp.int32, square, 0)
    corr[...] = jnp.zeros(corr.shape, jnp.float32)
    for r in range(HALF):
        at = pl.ds(r, nb, stride=HALF)
        x = jnp.concatenate([ens[0, at, :], ens[1, at, :]], axis=0)
        mean = jnp.sum(x, axis=1, keepdims=True) * (1.0 / members)
        x = (x - mean) * (1.0 / math.sqrt(members - 1))
        anom[r] = x
        full = dot(x, x, 1, 1)
        for delta in range(REACH + 1):
            corr[delta, r : r + 1, :] = jnp.sum(
                jnp.where(back == delta, full, 0.0), axis=0, keepdims=True
            )

    arrived(1)
    flat = pack[...].reshape(nb, LANES)
    turned = jnp.concatenate([flat, flat], axis=0).T
    on_lane = lax.broadcasted_iota(jnp.int32, tile, 1)
    obs_rows = jnp.where(on_lane < nb, turned[0:SUB], swap(turned[0:SUB]))
    inverse_obs = 1.0 / obs_rows
    chosen = [
        jnp.broadcast_to(turned[SUB + d : SUB + d + 1], tile) > 0.5 for d in range(REACH)
    ]
    at = SUB + REACH
    ridge = jnp.broadcast_to(turned[at : at + 1], tile)

    factor = {}
    inverse = []
    for j in range(REACH):
        for i in range(j, REACH):
            value = pltpu.roll(corr[i - j], j + 1, 1)
            running = jnp.where(chosen[j], jnp.where(chosen[i], value, 0.0), 0.0)
            if i == j:
                running = running + ridge
            for k in range(j):
                running = running - factor[i, k] * factor[j, k]
            if i == j:
                inverse.append(1.0 / jnp.sqrt(running))
            else:
                factor[i, j] = running * inverse[j]
    forward = []
    for i in range(REACH):
        running = jnp.where(chosen[i], corr[i + 1], 0.0)
        for k in range(i):
            running = running - factor[i, k] * forward[k]
        forward.append(running * inverse[i])
    beta = [None] * REACH
    for i in reversed(range(REACH)):
        running = forward[i]
        for k in range(i + 1, REACH):
            running = running - factor[k, i] * beta[k]
        beta[i] = running * inverse[i]

    lo = jnp.full((1, LANES), bounds[0], jnp.float32)
    hi = jnp.full((1, LANES), bounds[1], jnp.float32)
    theta = (hi + lo) / 2
    delta = (hi - lo) / 2
    sigma = theta / delta
    identity = jnp.where(back == 0, 1.0, 0.0)
    for r in range(HALF):
        upper = identity
        for d in range(REACH):
            upper = jnp.where(back == d + 1, -beta[d][r : r + 1], upper)
        resid = dot(anom[r], upper, 0, 0)
        inverse_var = 1.0 / (jnp.sum(resid * resid, axis=0, keepdims=True) + 1e-05)
        inverse_row = inverse_obs[r : r + 1]
        operator = dot(upper * inverse_var, upper, 1, 1) + jnp.where(back == 0, inverse_row, 0.0)
        rho = 1.0 / sigma
        direction = identity / theta
        total = direction
        residue = identity
        for step in range(ITERS):
            moved = operator / theta if step == 0 else dot(operator, direction, 1, 0)
            residue = residue - moved
            rho_next = 1.0 / (2 * sigma - rho)
            direction = rho_next * rho * direction + 2 * rho_next / delta * residue
            rho = rho_next
            total = total + direction
        filt[r] = total * inverse_row


def by_rows(n, ensemble, observed, obs_var, ridge, pred_back, bounds):
    local, rows, members = ensemble.shape
    nb = n * local
    f32 = jnp.float32
    vmem = pl.BlockSpec(memory_space=pltpu.VMEM)
    hbm = pl.BlockSpec(memory_space=pltpu.HBM)
    halves = pltpu.VMEM((2, n * SUB, members), f32)
    z = pl.pallas_call(
        functools.partial(whole_kernel, n),
        out_shape=jax.ShapeDtypeStruct(ensemble.shape, f32),
        in_specs=[hbm] * 6,
        out_specs=vmem,
        scratch_shapes=[
            pltpu.SMEM(bounds.shape, f32),
            pltpu.VMEM(ensemble.shape, f32),
            pltpu.VMEM(observed.shape, f32),
            pltpu.VMEM(obs_var.shape, f32),
            pltpu.SMEM(ridge.shape, f32),
            pltpu.SMEM(pred_back.shape, jnp.int32),
            pltpu.SemaphoreType.DMA((6,)),
            pltpu.VMEM((n, local, 1, LANES), f32),
            halves,
            halves,
            halves,
            halves,
            pltpu.VMEM((nb, 1, LANES), f32),
            halves,
            halves,
            pltpu.SemaphoreType.DMA((6,)),
            pltpu.SemaphoreType.DMA((6,)),
            pltpu.VMEM((HALF, LANES, LANES), f32),
            pltpu.VMEM((REACH + 1, SUB, LANES), f32),
            pltpu.VMEM((HALF, LANES, LANES), f32),
        ],
        compiler_params=pltpu.CompilerParams(
            collective_id=0, has_side_effects=True, vmem_limit_bytes=VMEM_GRANT
        ),
        name="whole",
    )(bounds, ensemble, observed, obs_var, ridge, pred_back)
    return ensemble + z


def choose(n, ensemble, *rest):
    local, rows, members = ensemble.shape
    even = lax.axis_size("blk") % 2 == 0 and local == 2
    if even and rows == n * SUB and members == LANES and 2 * n * local == LANES:
        return by_rows(n, ensemble, *rest)
    return on_device(ensemble, *rest)


def solution(mesh):
    return jax.shard_map(
        functools.partial(choose, mesh.size),
        mesh=mesh,
        in_specs=(
            P(("region", "blk"), None, None),
            P(("region", "blk"), None, None),
            P(("region", "blk"), None),
            P(("region", "blk")),
            P(("region", "blk"), None),
            P(),
        ),
        out_specs=P(("region", "blk"), None, None),
        check_vma=False,
    )
```

```python
import functools
import math

import jax
import jax.numpy as jnp
from jax import lax
from jax.experimental import pallas as pl
from jax.experimental.pallas import tpu as pltpu
from jax.sharding import PartitionSpec as P

REACH = 16
ITERS = 3


def from_behind(value, axis, steps):
    count = lax.axis_size(axis)
    first, last = (max(0, -steps), min(count, count - steps))
    return lax.ppermute(value, axis, [(source, source + steps) for source in range(first, last)])


def small_solve(gram, target):
    size = gram.shape[0]
    factor = {}
    for block_position in range(size):
        running = gram[block_position, block_position]
        for k in range(block_position):
            running = running - factor[block_position, k] * factor[block_position, k]
        factor[block_position, block_position] = jnp.sqrt(running)
        for i in range(block_position + 1, size):
            running = gram[i, block_position]
            for k in range(block_position):
                running = running - factor[i, k] * factor[block_position, k]
            factor[i, block_position] = running / factor[block_position, block_position]
    forward = []
    for i in range(size):
        running = target[i]
        for k in range(i):
            running = running - factor[i, k] * forward[k]
        forward.append(running / factor[i, i])
    analysis_output = [None] * size
    for i in reversed(range(size)):
        running = forward[i]
        for k in range(i + 1, size):
            running = running - factor[k, i] * analysis_output[k]
        analysis_output[i] = running / factor[i, i]
    return jnp.stack(analysis_output)


def previous_blocks(entry_values, reach_devices):
    pieces = [
        from_behind(entry_values, ("region", "blk"), shift_by)
        for shift_by in range(reach_devices, 0, -1)
    ]
    return jnp.concatenate(pieces, axis=0)


def on_device(ensemble, observed, obs_var, ridge, pred_back, bounds):
    highest = lax.Precision.HIGHEST
    local_blocks, rows, members = ensemble.shape
    slots = pred_back.shape[1]
    reach_devices = -(-REACH // local_blocks)
    before = reach_devices * local_blocks
    anomaly = (ensemble - jnp.mean(ensemble, axis=2, keepdims=True)) / jnp.sqrt(
        jnp.float32(members - 1)
    )
    positions = before + jnp.arange(local_blocks, dtype=jnp.int32)[:, None] - pred_back
    positions = jnp.where(pred_back > 0, positions, before + local_blocks)
    empty_zero_matrix = jnp.zeros((1, rows, members), jnp.float32)

    def extend(entry_values):
        return jnp.concatenate(
            [previous_blocks(entry_values, reach_devices), entry_values, empty_zero_matrix], axis=0
        )

    preds = extend(anomaly)[positions]
    identity = jnp.eye(slots, dtype=jnp.float32)
    gram = jnp.einsum("bjrm,bkrm->jkbr", preds, preds, precision=highest)
    gram = gram + ridge[None, None, :, None] * identity[:, :, None, None]
    target = jnp.einsum("bjrm,brm->jbr", preds, anomaly, precision=highest)
    regression_coefficients = small_solve(gram, target)
    resid = anomaly - jnp.einsum("jbr,bjrm->brm", regression_coefficients, preds, precision=highest)
    inverse_var = 1.0 / (jnp.sum(resid * resid, axis=2) + 1e-05)
    inverse_obs = 1.0 / obs_var
    beta_blocks = jnp.transpose(regression_coefficients, (1, 0, 2))
    lower_bound = bounds[0]
    upper_bound = bounds[1]
    theta = (upper_bound + lower_bound) / 2
    delta = (upper_bound - lower_bound) / 2
    sigma = theta / delta
    rho_now = 1.0 / sigma
    residue = inverse_obs[:, :, None] * (observed - ensemble)
    increment = jnp.zeros_like(ensemble)
    direction = residue / theta
    for step in range(ITERS):
        increment = increment + direction
        extended = extend(direction)
        lower_analysis_output = direction
        for lower_slot in range(slots):
            lower_analysis_output = (
                lower_analysis_output
                - beta_blocks[:, lower_slot, :, None] * extended[positions[:, lower_slot]]
            )
        upper_entry_values = lower_analysis_output * inverse_var[:, :, None]
        window = jnp.zeros((before + local_blocks + 1, rows, members), jnp.float32)
        for slot in range(slots):
            window = window.at[positions[:, slot]].add(
                beta_blocks[:, slot, :, None] * upper_entry_values
            )
        analysis_output = upper_entry_values - window[before : before + local_blocks]
        for shift_by in range(1, reach_devices + 1):
            start = (reach_devices - shift_by) * local_blocks
            analysis_output = analysis_output - from_behind(
                window[start : start + local_blocks], ("region", "blk"), -shift_by
            )
        residue = residue - (analysis_output + inverse_obs[:, :, None] * direction)
        rho_next = 1.0 / (2 * sigma - rho_now)
        direction = rho_next * rho_now * direction + 2 * rho_next / delta * residue
        rho_now = rho_next
    increment = increment + direction
    return ensemble + increment


VMEM_GRANT = 66_700_000
SUB = 8
HALF = SUB // 2
LANES = 128
MESH_ID = pl.DeviceIdType.MESH
HIGHEST = lax.Precision.HIGHEST


def place():
    per = lax.axis_size("blk")
    region, blk = lax.axis_index("region"), lax.axis_index("blk")
    return lax.axis_size("region"), per, region, blk, region * per + blk


def each_peer(where, visit):
    regions, per, region, blk, me = where
    n = regions * per
    def step(i, carry):
        k = lax.rem(me + i, n)
        visit((k // per, lax.rem(k, per)), k)
        return carry
    lax.fori_loop(1, n, step, 0)


def copy_to(src, dst, send_sem, recv_sem, device):
    return pltpu.make_async_remote_copy(
        src_ref=src,
        dst_ref=dst,
        send_sem=send_sem,
        recv_sem=recv_sem,
        device_id=device,
        device_id_type=MESH_ID,
    )


def tile_at(k):
    return pl.ds(pl.multiple_of(k * SUB, SUB), SUB)


def swap(x):
    return pltpu.roll(x, HALF, 0)


def pair_rows(n, src, dst):
    low = lax.broadcasted_iota(jnp.int32, (SUB, LANES), 0) < HALF
    for k in range(n):
        at = slice(k * SUB, (k + 1) * SUB)
        first, second = src[0, at, :], src[1, at, :]
        dst[0, at, :] = jnp.where(low, first, swap(second))
        dst[1, at, :] = jnp.where(low, swap(first), second)


def fill_pack(rows, obs_var, ridge, pred_back, pack):
    local = pred_back.shape[0]
    lane = lax.broadcasted_iota(jnp.int32, (1, LANES), 1)
    groups = LANES // SUB
    for block in range(local):
        meta = jnp.where(lane == SUB + REACH, ridge[block], 0.0)
        for slot in range(pred_back.shape[1]):
            back = pred_back[block, slot]
            meta = jnp.where((lane == back + (SUB - 1)) & (lane >= SUB), 1.0, meta)
        for part in range(rows // LANES):
            row = obs_var[block : block + 1, part * LANES : (part + 1) * LANES]
            for k in range(groups):
                turned = row if k == 0 else pltpu.roll(row, LANES - SUB * k, 1)
                pack[part * groups + k, block] = jnp.where(lane < SUB, turned, meta)


def whole_kernel(
    n, bounds_in, ens_in, obs_in, obs_var_in, ridge_in, pred_back_in, z,
    bounds, ens, obs, obs_var, ridge, pred_back, load_sem,
    pack, obs_s, ens_r, obs_r, pack_r, z_s, z_r, send_sem, recv_sem,
    corr, filt,
):
    where = place()
    me = where[-1]
    local, rows, members = ens.shape
    loads = [
        pltpu.make_async_copy(src, dst, load_sem.at[i])
        for i, (src, dst) in enumerate(
            (
                (ens_in, ens),
                (obs_in, obs),
                (obs_var_in, obs_var),
                (ridge_in, ridge),
                (pred_back_in, pred_back),
                (bounds_in, bounds),
            )
        )
    ]
    for load in loads:
        load.start()
    barrier = pltpu.get_barrier_semaphore()

    def signal(device, k):
        pl.semaphore_signal(barrier, inc=1, device_id=device, device_id_type=MESH_ID)

    each_peer(where, signal)
    own = tile_at(me)
    mine = pl.ds(me * local, local)
    loads[0].wait()
    pl.semaphore_wait(barrier, n - 1)

    def send_ens(device, k):
        copy_to(
            ens.at[:, tile_at(k), :], ens_r.at[mine], send_sem.at[0], recv_sem.at[0], device
        ).start()

    def send_pack(device, k):
        copy_to(pack.at[k], pack_r.at[mine], send_sem.at[1], recv_sem.at[1], device).start()

    def send_half(src, dst, h, which):
        def send(device, k):
            copy_to(
                src.at[h, tile_at(k), :], dst.at[h, own, :], send_sem.at[which], recv_sem.at[which],
                device,
            ).start()

        return send

    each_peer(where, send_ens)
    for load in loads[1:]:
        load.wait()
    fill_pack(rows, obs_var, ridge, pred_back, pack)
    each_peer(where, send_pack)
    pair_rows(n, obs, obs_s)
    each_peer(where, send_half(obs_s, obs_r, 0, 2))
    each_peer(where, send_half(obs_s, obs_r, 1, 3))

    ens_r[mine] = ens[:, own, :]
    pack_r[mine] = pack[me]
    obs_r[:, own, :] = obs_s[:, own, :]
    others = pl.ds(0, (n - 1) * SUB)
    whole = (
        ens_r.at[pl.ds(0, (n - 1) * local)],
        pack_r.at[pl.ds(0, (n - 1) * local)],
        obs_r.at[0, others, :],
        obs_r.at[1, others, :],
        z_r.at[0, others, :],
        z_r.at[1, others, :],
    )
    regions, per, region, blk, unused = where
    neighbour = (lax.rem(region + 1, regions), blk)

    def arrived(which):
        ref = whole[which]
        copy_to(ref, ref, send_sem.at[which], recv_sem.at[which], neighbour).wait_recv()

    arrived(0)
    make_filters(n * local, arrived, bounds, ens_r, pack_r, corr, filt)
    nb = n * local
    empty = jnp.zeros((nb, members), jnp.float32)
    for h in range(2):
        arrived(2 + h)
        for pair in range(HALF // 2):
            gaps = [
                obs_r[h, pl.ds(r, nb, stride=HALF), :] - ens_r[pl.ds(0, nb), h * HALF + r, :]
                for r in (2 * pair, 2 * pair + 1)
            ]
            columns = []
            for r in range(2):
                column = [empty] * 4
                column[2 * r + h] = gaps[r]
                columns.append(jnp.concatenate(column, axis=0))
            found = dot(filt[pair], jnp.concatenate(columns, axis=1), 1, 0)
            for r in range(2):
                z_s[h, pl.ds(2 * pair + r, nb, stride=HALF), :] = found[
                    :, r * members : (r + 1) * members
                ]
        each_peer(where, send_half(z_s, z_r, h, 4 + h))
        z_r[h, own, :] = z_s[h, own, :]
    low = lax.broadcasted_iota(jnp.int32, (SUB, LANES), 0) < HALF
    arrived(4)
    arrived(5)
    for k in range(n):
        at = slice(k * SUB, (k + 1) * SUB)
        first, second = z_r[0, at, :], z_r[1, at, :]
        z[0, at, :] = jnp.where(low, first, swap(second))
        z[1, at, :] = jnp.where(low, swap(first), second)
    for which, ref in enumerate(whole):
        copy_to(ref, ref, send_sem.at[which], recv_sem.at[which], neighbour).wait_send()


def dot(lhs, rhs, left, right):
    return lax.dot_general(
        lhs,
        rhs,
        (((left,), (right,)), ((), ())),
        precision=HIGHEST,
        preferred_element_type=jnp.float32,
    )


def spread(x, on):
    return jnp.where(on, jnp.concatenate([x] * (x.shape[1] // x.shape[0]), axis=0), 0.0)


def make_filters(nb, arrived, bounds, ens, pack, corr, filt):
    members = ens.shape[2]
    tile = (SUB, LANES)
    wide = 2 * LANES
    back = lax.rem(lax.broadcasted_iota(jnp.int32, (nb, LANES), 1), nb) - lax.broadcasted_iota(
        jnp.int32, (nb, LANES), 0
    )
    on = lax.broadcasted_iota(jnp.int32, (wide, wide), 0) // nb == lax.broadcasted_iota(
        jnp.int32, (wide, wide), 1
    ) // nb
    empty = jnp.zeros((nb, members), jnp.float32)
    corr[...] = jnp.zeros(corr.shape, jnp.float32)
    anom = []
    for r in range(HALF):
        sides = []
        for h in range(2):
            x = ens[pl.ds(0, nb), h * HALF + r, :]
            mean = jnp.sum(x, axis=1, keepdims=True) * (1.0 / members)
            sides.append((x - mean) * (1.0 / math.sqrt(members - 1)))
        anom.append(jnp.concatenate(sides, axis=0))
        rhs = jnp.concatenate(
            [
                jnp.concatenate([sides[0], empty], axis=1),
                jnp.concatenate([empty, sides[1]], axis=1),
            ],
            axis=0,
        )
        full = dot(jnp.concatenate(sides, axis=1), rhs, 1, 1)
        for delta in range(REACH + 1):
            corr[delta, r : r + 1, :] = jnp.sum(
                jnp.where(back == delta, full, 0.0), axis=0, keepdims=True
            )

    arrived(1)
    flat = pack[...].reshape(nb, LANES)
    turned = jnp.concatenate([flat, flat], axis=0).T
    on_lane = lax.broadcasted_iota(jnp.int32, tile, 1)
    obs_rows = jnp.where(on_lane < nb, turned[0:SUB], swap(turned[0:SUB]))
    inverse_obs = 1.0 / obs_rows
    chosen = [
        jnp.broadcast_to(turned[SUB + d : SUB + d + 1], tile) > 0.5 for d in range(REACH)
    ]
    at = SUB + REACH
    ridge = jnp.broadcast_to(turned[at : at + 1], tile)

    factor = {}
    inverse = []
    for j in range(REACH):
        for i in range(j, REACH):
            value = pltpu.roll(corr[i - j], j + 1, 1)
            running = jnp.where(chosen[j], jnp.where(chosen[i], value, 0.0), 0.0)
            if i == j:
                running = running + ridge
            for k in range(j):
                running = running - factor[i, k] * factor[j, k]
            if i == j:
                inverse.append(1.0 / jnp.sqrt(running))
            else:
                factor[i, j] = running * inverse[j]
    forward = []
    for i in range(REACH):
        running = jnp.where(chosen[i], corr[i + 1], 0.0)
        for k in range(i):
            running = running - factor[i, k] * forward[k]
        forward.append(running * inverse[i])
    beta = [None] * REACH
    for i in reversed(range(REACH)):
        running = forward[i]
        for k in range(i + 1, REACH):
            running = running - factor[k, i] * beta[k]
        beta[i] = running * inverse[i]

    lo = jnp.full((1, wide), bounds[0], jnp.float32)
    hi = jnp.full((1, wide), bounds[1], jnp.float32)
    theta = (hi + lo) / 2
    delta = (hi - lo) / 2
    sigma = theta / delta
    here = back == 0
    identity = jnp.where(jnp.concatenate([here, here], axis=1), 1.0, 0.0)
    pairs = range(HALF // 2)
    rows = lambda pair: (2 * pair, 2 * pair + 1)
    inverse_row = [
        jnp.concatenate([inverse_obs[r : r + 1] for r in rows(pair)], axis=1) for pair in pairs
    ]
    upper = []
    for pair in pairs:
        sides = []
        for r in rows(pair):
            side = jnp.where(here, 1.0, 0.0)
            for d in range(REACH):
                side = jnp.where(back == d + 1, -beta[d][r : r + 1], side)
            sides.append(side)
        upper.append(jnp.concatenate(sides, axis=1))
    spread_upper = [spread(x, on) for x in upper]
    resid = [
        dot(jnp.concatenate([anom[r] for r in rows(pair)], axis=0), spread_upper[pair], 0, 0)
        for pair in pairs
    ]
    inverse_var = [1.0 / (jnp.sum(x * x, axis=0, keepdims=True) + 1e-05) for x in resid]
    operator = [
        dot(upper[pair] * inverse_var[pair], spread_upper[pair], 1, 1)
        + identity * inverse_row[pair]
        for pair in pairs
    ]
    spread_operator = [spread(x, on) for x in operator]
    rho = 1.0 / sigma
    direction = [identity / theta for pair in pairs]
    total = direction
    residue = [identity for pair in pairs]
    for step in range(ITERS):
        moved = [
            operator[pair] / theta if step == 0 else dot(direction[pair], spread_operator[pair], 1, 0)
            for pair in pairs
        ]
        residue = [residue[pair] - moved[pair] for pair in pairs]
        rho_next = 1.0 / (2 * sigma - rho)
        keep = rho_next * rho
        move = 2 * rho_next / delta
        rho = rho_next
        direction = [keep * direction[pair] + move * residue[pair] for pair in pairs]
        total = [total[pair] + direction[pair] for pair in pairs]
    for pair in pairs:
        filt[pair] = total[pair] * inverse_row[pair]


def by_rows(n, ensemble, observed, obs_var, ridge, pred_back, bounds):
    local, rows, members = ensemble.shape
    nb = n * local
    f32 = jnp.float32
    vmem = pl.BlockSpec(memory_space=pltpu.VMEM)
    hbm = pl.BlockSpec(memory_space=pltpu.HBM)
    halves = pltpu.VMEM((2, n * SUB, members), f32)
    z = pl.pallas_call(
        functools.partial(whole_kernel, n),
        out_shape=jax.ShapeDtypeStruct(ensemble.shape, f32),
        in_specs=[hbm] * 6,
        out_specs=vmem,
        scratch_shapes=[
            pltpu.SMEM(bounds.shape, f32),
            pltpu.VMEM(ensemble.shape, f32),
            pltpu.VMEM(observed.shape, f32),
            pltpu.VMEM(obs_var.shape, f32),
            pltpu.SMEM(ridge.shape, f32),
            pltpu.SMEM(pred_back.shape, jnp.int32),
            pltpu.SemaphoreType.DMA((6,)),
            pltpu.VMEM((n, local, 1, LANES), f32),
            halves,
            pltpu.VMEM((nb, SUB, members), f32),
            halves,
            pltpu.VMEM((nb, 1, LANES), f32),
            halves,
            halves,
            pltpu.SemaphoreType.DMA((6,)),
            pltpu.SemaphoreType.DMA((6,)),
            pltpu.VMEM((REACH + 1, SUB, LANES), f32),
            pltpu.VMEM((HALF // 2, nb, 2 * LANES), f32),
        ],
        compiler_params=pltpu.CompilerParams(
            collective_id=0, has_side_effects=True, vmem_limit_bytes=VMEM_GRANT
        ),
        name="whole",
    )(bounds, ensemble, observed, obs_var, ridge, pred_back)
    return ensemble + z


def choose(n, ensemble, *rest):
    local, rows, members = ensemble.shape
    even = lax.axis_size("blk") % 2 == 0 and local == 2
    if even and rows == n * SUB and members == LANES and 2 * n * local == LANES:
        return by_rows(n, ensemble, *rest)
    return on_device(ensemble, *rest)


def solution(mesh):
    return jax.shard_map(
        functools.partial(choose, mesh.size),
        mesh=mesh,
        in_specs=(
            P(("region", "blk"), None, None),
            P(("region", "blk"), None, None),
            P(("region", "blk"), None),
            P(("region", "blk")),
            P(("region", "blk"), None),
            P(),
        ),
        out_specs=P(("region", "blk"), None, None),
        check_vma=False,
    )
```

```python
import functools
import math

import jax
import jax.numpy as jnp
from jax import lax
from jax.experimental import pallas as pl
from jax.experimental.pallas import tpu as pltpu
from jax.sharding import PartitionSpec as P

REACH = 16
ITERS = 3


def from_behind(value, axis, steps):
    count = lax.axis_size(axis)
    first, last = (max(0, -steps), min(count, count - steps))
    return lax.ppermute(value, axis, [(source, source + steps) for source in range(first, last)])


def small_solve(gram, target):
    size = gram.shape[0]
    factor = {}
    for block_position in range(size):
        running = gram[block_position, block_position]
        for k in range(block_position):
            running = running - factor[block_position, k] * factor[block_position, k]
        factor[block_position, block_position] = jnp.sqrt(running)
        for i in range(block_position + 1, size):
            running = gram[i, block_position]
            for k in range(block_position):
                running = running - factor[i, k] * factor[block_position, k]
            factor[i, block_position] = running / factor[block_position, block_position]
    forward = []
    for i in range(size):
        running = target[i]
        for k in range(i):
            running = running - factor[i, k] * forward[k]
        forward.append(running / factor[i, i])
    analysis_output = [None] * size
    for i in reversed(range(size)):
        running = forward[i]
        for k in range(i + 1, size):
            running = running - factor[k, i] * analysis_output[k]
        analysis_output[i] = running / factor[i, i]
    return jnp.stack(analysis_output)


def previous_blocks(entry_values, reach_devices):
    pieces = [
        from_behind(entry_values, ("region", "blk"), shift_by)
        for shift_by in range(reach_devices, 0, -1)
    ]
    return jnp.concatenate(pieces, axis=0)


def on_device(ensemble, observed, obs_var, ridge, pred_back, bounds):
    highest = lax.Precision.HIGHEST
    local_blocks, rows, members = ensemble.shape
    slots = pred_back.shape[1]
    reach_devices = -(-REACH // local_blocks)
    before = reach_devices * local_blocks
    anomaly = (ensemble - jnp.mean(ensemble, axis=2, keepdims=True)) / jnp.sqrt(
        jnp.float32(members - 1)
    )
    positions = before + jnp.arange(local_blocks, dtype=jnp.int32)[:, None] - pred_back
    positions = jnp.where(pred_back > 0, positions, before + local_blocks)
    empty_zero_matrix = jnp.zeros((1, rows, members), jnp.float32)

    def extend(entry_values):
        return jnp.concatenate(
            [previous_blocks(entry_values, reach_devices), entry_values, empty_zero_matrix], axis=0
        )

    preds = extend(anomaly)[positions]
    identity = jnp.eye(slots, dtype=jnp.float32)
    gram = jnp.einsum("bjrm,bkrm->jkbr", preds, preds, precision=highest)
    gram = gram + ridge[None, None, :, None] * identity[:, :, None, None]
    target = jnp.einsum("bjrm,brm->jbr", preds, anomaly, precision=highest)
    regression_coefficients = small_solve(gram, target)
    resid = anomaly - jnp.einsum("jbr,bjrm->brm", regression_coefficients, preds, precision=highest)
    inverse_var = 1.0 / (jnp.sum(resid * resid, axis=2) + 1e-05)
    inverse_obs = 1.0 / obs_var
    beta_blocks = jnp.transpose(regression_coefficients, (1, 0, 2))
    lower_bound = bounds[0]
    upper_bound = bounds[1]
    theta = (upper_bound + lower_bound) / 2
    delta = (upper_bound - lower_bound) / 2
    sigma = theta / delta
    rho_now = 1.0 / sigma
    residue = inverse_obs[:, :, None] * (observed - ensemble)
    increment = jnp.zeros_like(ensemble)
    direction = residue / theta
    for step in range(ITERS):
        increment = increment + direction
        extended = extend(direction)
        lower_analysis_output = direction
        for lower_slot in range(slots):
            lower_analysis_output = (
                lower_analysis_output
                - beta_blocks[:, lower_slot, :, None] * extended[positions[:, lower_slot]]
            )
        upper_entry_values = lower_analysis_output * inverse_var[:, :, None]
        window = jnp.zeros((before + local_blocks + 1, rows, members), jnp.float32)
        for slot in range(slots):
            window = window.at[positions[:, slot]].add(
                beta_blocks[:, slot, :, None] * upper_entry_values
            )
        analysis_output = upper_entry_values - window[before : before + local_blocks]
        for shift_by in range(1, reach_devices + 1):
            start = (reach_devices - shift_by) * local_blocks
            analysis_output = analysis_output - from_behind(
                window[start : start + local_blocks], ("region", "blk"), -shift_by
            )
        residue = residue - (analysis_output + inverse_obs[:, :, None] * direction)
        rho_next = 1.0 / (2 * sigma - rho_now)
        direction = rho_next * rho_now * direction + 2 * rho_next / delta * residue
        rho_now = rho_next
    increment = increment + direction
    return ensemble + increment


VMEM_GRANT = 48_000_000
SUB = 8
HALF = SUB // 2
LANES = 128
PLANES = 4
MESH_ID = pl.DeviceIdType.MESH
HIGHEST = lax.Precision.HIGHEST


def place():
    per = lax.axis_size("blk")
    region, blk = lax.axis_index("region"), lax.axis_index("blk")
    return lax.axis_size("region"), per, region, blk, region * per + blk


def peer(where, up, j):
    regions, per, region, blk, unused = where
    depth = per // PLANES
    plane = lax.rem(blk // depth + up, PLANES)
    at = lax.rem(region * depth + lax.rem(blk, depth) + j, regions * depth)
    to, blk_to = at // depth, plane * depth + lax.rem(at, depth)
    return (to, blk_to), to * per + blk_to


def each_peer(where, visit, before=lambda up: None):
    width = where[0] * where[1] // PLANES
    for up in range(PLANES):
        before(up)

        def step(j, carry, up=up):
            visit(*peer(where, up, j))
            return carry

        lax.fori_loop(0 if up else 1, width, step, 0)


def copy_to(src, dst, send_sem, recv_sem, device):
    return pltpu.make_async_remote_copy(
        src_ref=src,
        dst_ref=dst,
        send_sem=send_sem,
        recv_sem=recv_sem,
        device_id=device,
        device_id_type=MESH_ID,
    )


def tile_at(k):
    return pl.ds(pl.multiple_of(k * SUB, SUB), SUB)


def swap(x):
    return pltpu.roll(x, HALF, 0)


def pair_rows(n, src, dst):
    low = lax.broadcasted_iota(jnp.int32, (SUB, LANES), 0) < HALF
    for k in range(n):
        at = slice(k * SUB, (k + 1) * SUB)
        first, second = src[0, at, :], src[1, at, :]
        dst[0, at, :] = jnp.where(low, first, swap(second))
        dst[1, at, :] = jnp.where(low, swap(first), second)


def fill_pack(rows, obs_var, ridge, pred_back, pack):
    local = pred_back.shape[0]
    lane = lax.broadcasted_iota(jnp.int32, (1, LANES), 1)
    groups = LANES // SUB
    for block in range(local):
        meta = jnp.where(lane == SUB + REACH, ridge[block], 0.0)
        for slot in range(pred_back.shape[1]):
            back = pred_back[block, slot]
            meta = jnp.where((lane == back + (SUB - 1)) & (lane >= SUB), 1.0, meta)
        for part in range(rows // LANES):
            row = obs_var[block : block + 1, part * LANES : (part + 1) * LANES]
            for k in range(groups):
                turned = row if k == 0 else pltpu.roll(row, LANES - SUB * k, 1)
                pack[part * groups + k, block] = jnp.where(lane < SUB, turned, meta)


def whole_kernel(
    n, bounds_in, ens_in, obs_in, obs_var_in, ridge_in, pred_back_in, z,
    bounds, ens, obs, obs_var, ridge, pred_back, load_sem,
    pack, obs_s, ens_r, obs_r, pack_r, z_s, z_r, ready, send_sem, recv_sem,
    corr, filt,
):
    where = place()
    me = where[-1]
    local, rows, members = ens.shape
    loads = [
        pltpu.make_async_copy(src, dst, load_sem.at[i])
        for i, (src, dst) in enumerate(
            (
                (ens_in, ens),
                (obs_in, obs),
                (obs_var_in, obs_var),
                (ridge_in, ridge),
                (pred_back_in, pred_back),
                (bounds_in, bounds),
            )
        )
    ]
    for load in loads:
        load.start()
    barrier = pltpu.get_barrier_semaphore()


    def signal(sem, up, j):
        device, unused = peer(where, up, j)
        pl.semaphore_signal(sem, inc=1, device_id=device, device_id_type=MESH_ID)

    width = n // PLANES
    for up in range(1, PLANES):
        signal(barrier, up, 0)
    for j in range(1, width):
        signal(barrier, 0, j)
    own = tile_at(me)
    mine = pl.ds(me * local, local)
    pl.semaphore_wait(barrier, width - 1 + PLANES - 1)
    for up in range(1, PLANES):
        signal(ready.at[PLANES - up], up, 0)
    loads[0].wait()

    def plane_ready(up):
        if up:
            pl.semaphore_wait(ready.at[up], 1)

    def send_ens(device, k):
        copy_to(
            ens.at[:, tile_at(k), :], ens_r.at[mine], send_sem.at[0], recv_sem.at[0], device
        ).start()

    def send_pack(device, k):
        copy_to(pack.at[k], pack_r.at[mine], send_sem.at[1], recv_sem.at[1], device).start()

    def send_half(src, dst, h, which):
        def send(device, k):
            copy_to(
                src.at[h, tile_at(k), :], dst.at[h, own, :], send_sem.at[which], recv_sem.at[which],
                device,
            ).start()

        return send

    each_peer(where, send_ens, plane_ready)
    for load in loads[1:]:
        load.wait()
    fill_pack(rows, obs_var, ridge, pred_back, pack)
    each_peer(where, send_pack)
    pair_rows(n, obs, obs_s)
    each_peer(where, send_half(obs_s, obs_r, 0, 2))
    each_peer(where, send_half(obs_s, obs_r, 1, 3))

    ens_r[mine] = ens[:, own, :]
    pack_r[mine] = pack[me]
    obs_r[:, own, :] = obs_s[:, own, :]
    others = pl.ds(0, (n - 1) * SUB)
    whole = (
        ens_r.at[pl.ds(0, (n - 1) * local)],
        pack_r.at[pl.ds(0, (n - 1) * local)],
        obs_r.at[0, others, :],
        obs_r.at[1, others, :],
        z_r.at[0, others, :],
        z_r.at[1, others, :],
    )
    regions, per, region, blk, unused = where
    neighbour = (lax.rem(region + 1, regions), blk)

    def arrived(which):
        ref = whole[which]
        copy_to(ref, ref, send_sem.at[which], recv_sem.at[which], neighbour).wait_recv()

    arrived(0)
    make_filters(n * local, arrived, bounds, ens_r, pack_r, corr, filt)
    nb = n * local
    empty = jnp.zeros((nb, members), jnp.float32)
    for h in range(2):
        arrived(2 + h)
        for pair in range(HALF // 2):
            gaps = [
                obs_r[h, pl.ds(r, nb, stride=HALF), :] - ens_r[pl.ds(0, nb), h * HALF + r, :]
                for r in (2 * pair, 2 * pair + 1)
            ]
            columns = []
            for r in range(2):
                column = [empty] * 4
                column[2 * r + h] = gaps[r]
                columns.append(jnp.concatenate(column, axis=0))
            found = dot(filt[pair], jnp.concatenate(columns, axis=1), 1, 0)
            for r in range(2):
                z_s[h, pl.ds(2 * pair + r, nb, stride=HALF), :] = found[
                    :, r * members : (r + 1) * members
                ]
        each_peer(where, send_half(z_s, z_r, h, 4 + h))
        z_r[h, own, :] = z_s[h, own, :]
    low = lax.broadcasted_iota(jnp.int32, (SUB, LANES), 0) < HALF
    arrived(4)
    arrived(5)
    for k in range(n):
        at = slice(k * SUB, (k + 1) * SUB)
        first, second = z_r[0, at, :], z_r[1, at, :]
        z[0, at, :] = jnp.where(low, first, swap(second))
        z[1, at, :] = jnp.where(low, swap(first), second)
    for which, ref in enumerate(whole):
        copy_to(ref, ref, send_sem.at[which], recv_sem.at[which], neighbour).wait_send()


def dot(lhs, rhs, left, right):
    return lax.dot_general(
        lhs,
        rhs,
        (((left,), (right,)), ((), ())),
        precision=HIGHEST,
        preferred_element_type=jnp.float32,
    )


def spread(x, on):
    return jnp.where(on, jnp.concatenate([x] * (x.shape[1] // x.shape[0]), axis=0), 0.0)


def make_filters(nb, arrived, bounds, ens, pack, corr, filt):
    members = ens.shape[2]
    tile = (SUB, LANES)
    wide = 2 * LANES
    back = lax.rem(lax.broadcasted_iota(jnp.int32, (nb, LANES), 1), nb) - lax.broadcasted_iota(
        jnp.int32, (nb, LANES), 0
    )
    on = lax.broadcasted_iota(jnp.int32, (wide, wide), 0) // nb == lax.broadcasted_iota(
        jnp.int32, (wide, wide), 1
    ) // nb
    empty = jnp.zeros((nb, members), jnp.float32)
    corr[...] = jnp.zeros(corr.shape, jnp.float32)
    anom = []
    for r in range(HALF):
        sides = []
        for h in range(2):
            x = ens[pl.ds(0, nb), h * HALF + r, :]
            mean = jnp.sum(x, axis=1, keepdims=True) * (1.0 / members)
            sides.append((x - mean) * (1.0 / math.sqrt(members - 1)))
        anom.append(jnp.concatenate(sides, axis=0))
        rhs = jnp.concatenate(
            [
                jnp.concatenate([sides[0], empty], axis=1),
                jnp.concatenate([empty, sides[1]], axis=1),
            ],
            axis=0,
        )
        full = dot(jnp.concatenate(sides, axis=1), rhs, 1, 1)
        for delta in range(REACH + 1):
            corr[delta, r : r + 1, :] = jnp.sum(
                jnp.where(back == delta, full, 0.0), axis=0, keepdims=True
            )

    arrived(1)
    flat = pack[...].reshape(nb, LANES)
    turned = jnp.concatenate([flat, flat], axis=0).T
    on_lane = lax.broadcasted_iota(jnp.int32, tile, 1)
    obs_rows = jnp.where(on_lane < nb, turned[0:SUB], swap(turned[0:SUB]))
    inverse_obs = 1.0 / obs_rows
    chosen = [
        jnp.broadcast_to(turned[SUB + d : SUB + d + 1], tile) > 0.5 for d in range(REACH)
    ]
    at = SUB + REACH
    ridge = jnp.broadcast_to(turned[at : at + 1], tile)

    factor = {}
    inverse = []
    for j in range(REACH):
        for i in range(j, REACH):
            value = pltpu.roll(corr[i - j], j + 1, 1)
            running = jnp.where(chosen[j], jnp.where(chosen[i], value, 0.0), 0.0)
            if i == j:
                running = running + ridge
            for k in range(j):
                running = running - factor[i, k] * factor[j, k]
            if i == j:
                inverse.append(1.0 / jnp.sqrt(running))
            else:
                factor[i, j] = running * inverse[j]
    forward = []
    for i in range(REACH):
        running = jnp.where(chosen[i], corr[i + 1], 0.0)
        for k in range(i):
            running = running - factor[i, k] * forward[k]
        forward.append(running * inverse[i])
    beta = [None] * REACH
    for i in reversed(range(REACH)):
        running = forward[i]
        for k in range(i + 1, REACH):
            running = running - factor[k, i] * beta[k]
        beta[i] = running * inverse[i]

    lo = jnp.full((1, wide), bounds[0], jnp.float32)
    hi = jnp.full((1, wide), bounds[1], jnp.float32)
    theta = (hi + lo) / 2
    delta = (hi - lo) / 2
    sigma = theta / delta
    here = back == 0
    identity = jnp.where(jnp.concatenate([here, here], axis=1), 1.0, 0.0)
    pairs = range(HALF // 2)
    rows = lambda pair: (2 * pair, 2 * pair + 1)
    inverse_row = [
        jnp.concatenate([inverse_obs[r : r + 1] for r in rows(pair)], axis=1) for pair in pairs
    ]
    upper = []
    for pair in pairs:
        sides = []
        for r in rows(pair):
            side = jnp.where(here, 1.0, 0.0)
            for d in range(REACH):
                side = jnp.where(back == d + 1, -beta[d][r : r + 1], side)
            sides.append(side)
        upper.append(jnp.concatenate(sides, axis=1))
    spread_upper = [spread(x, on) for x in upper]
    resid = [
        dot(jnp.concatenate([anom[r] for r in rows(pair)], axis=0), spread_upper[pair], 0, 0)
        for pair in pairs
    ]
    inverse_var = [1.0 / (jnp.sum(x * x, axis=0, keepdims=True) + 1e-05) for x in resid]
    operator = [
        dot(upper[pair] * inverse_var[pair], spread_upper[pair], 1, 1)
        + identity * inverse_row[pair]
        for pair in pairs
    ]
    spread_operator = [spread(x, on) for x in operator]
    rho = 1.0 / sigma
    direction = [identity / theta for pair in pairs]
    total = direction
    residue = [identity for pair in pairs]
    for step in range(ITERS):
        moved = [
            operator[pair] / theta if step == 0 else dot(direction[pair], spread_operator[pair], 1, 0)
            for pair in pairs
        ]
        residue = [residue[pair] - moved[pair] for pair in pairs]
        rho_next = 1.0 / (2 * sigma - rho)
        keep = rho_next * rho
        move = 2 * rho_next / delta
        rho = rho_next
        direction = [keep * direction[pair] + move * residue[pair] for pair in pairs]
        total = [total[pair] + direction[pair] for pair in pairs]
    for pair in pairs:
        filt[pair] = total[pair] * inverse_row[pair]


def by_rows(n, ensemble, observed, obs_var, ridge, pred_back, bounds):
    local, rows, members = ensemble.shape
    nb = n * local
    f32 = jnp.float32
    vmem = pl.BlockSpec(memory_space=pltpu.VMEM)
    hbm = pl.BlockSpec(memory_space=pltpu.HBM)
    halves = pltpu.VMEM((2, n * SUB, members), f32)
    z = pl.pallas_call(
        functools.partial(whole_kernel, n),
        out_shape=pltpu.VMEM(ensemble.shape, f32),
        in_specs=[hbm] * 6,
        out_specs=vmem,
        scratch_shapes=[
            pltpu.SMEM(bounds.shape, f32),
            pltpu.VMEM(ensemble.shape, f32),
            pltpu.VMEM(observed.shape, f32),
            pltpu.VMEM(obs_var.shape, f32),
            pltpu.SMEM(ridge.shape, f32),
            pltpu.SMEM(pred_back.shape, jnp.int32),
            pltpu.SemaphoreType.DMA((6,)),
            pltpu.VMEM((n, local, 1, LANES), f32),
            halves,
            pltpu.VMEM((nb, SUB, members), f32),
            halves,
            pltpu.VMEM((nb, 1, LANES), f32),
            halves,
            halves,
            pltpu.SemaphoreType.REGULAR((PLANES,)),
            pltpu.SemaphoreType.DMA((6,)),
            pltpu.SemaphoreType.DMA((6,)),
            pltpu.VMEM((REACH + 1, SUB, LANES), f32),
            pltpu.VMEM((HALF // 2, nb, 2 * LANES), f32),
        ],
        compiler_params=pltpu.CompilerParams(
            collective_id=0, has_side_effects=True, vmem_limit_bytes=VMEM_GRANT
        ),
        name="whole",
    )(*[
        pltpu.with_memory_space_constraint(x, pltpu.HBM)
        for x in (bounds, ensemble, observed, obs_var, ridge, pred_back)
    ])
    return ensemble + z


def choose(n, ensemble, *rest):
    local, rows, members = ensemble.shape
    even = lax.axis_size("blk") % PLANES == 0 and local == 2
    if even and rows == n * SUB and members == LANES and 2 * n * local == LANES:
        return by_rows(n, ensemble, *rest)
    return on_device(ensemble, *rest)


def solution(mesh):
    return jax.shard_map(
        functools.partial(choose, mesh.size),
        mesh=mesh,
        in_specs=(
            P(("region", "blk"), None, None),
            P(("region", "blk"), None, None),
            P(("region", "blk"), None),
            P(("region", "blk")),
            P(("region", "blk"), None),
            P(),
        ),
        out_specs=P(("region", "blk"), None, None),
        check_vma=False,
    )
```

```python
import functools
import math

import jax
import jax.numpy as jnp
from jax import lax
from jax.experimental import pallas as pl
from jax.experimental.pallas import tpu as pltpu
from jax.sharding import PartitionSpec as P

REACH = 16
ITERS = 3


def from_behind(value, axis, steps):
    count = lax.axis_size(axis)
    first, last = (max(0, -steps), min(count, count - steps))
    return lax.ppermute(value, axis, [(source, source + steps) for source in range(first, last)])


def small_solve(gram, target):
    size = gram.shape[0]
    factor = {}
    for block_position in range(size):
        running = gram[block_position, block_position]
        for k in range(block_position):
            running = running - factor[block_position, k] * factor[block_position, k]
        factor[block_position, block_position] = jnp.sqrt(running)
        for i in range(block_position + 1, size):
            running = gram[i, block_position]
            for k in range(block_position):
                running = running - factor[i, k] * factor[block_position, k]
            factor[i, block_position] = running / factor[block_position, block_position]
    forward = []
    for i in range(size):
        running = target[i]
        for k in range(i):
            running = running - factor[i, k] * forward[k]
        forward.append(running / factor[i, i])
    analysis_output = [None] * size
    for i in reversed(range(size)):
        running = forward[i]
        for k in range(i + 1, size):
            running = running - factor[k, i] * analysis_output[k]
        analysis_output[i] = running / factor[i, i]
    return jnp.stack(analysis_output)


def previous_blocks(entry_values, reach_devices):
    pieces = [
        from_behind(entry_values, ("region", "blk"), shift_by)
        for shift_by in range(reach_devices, 0, -1)
    ]
    return jnp.concatenate(pieces, axis=0)


def on_device(ensemble, observed, obs_var, ridge, pred_back, bounds):
    highest = lax.Precision.HIGHEST
    local_blocks, rows, members = ensemble.shape
    slots = pred_back.shape[1]
    reach_devices = -(-REACH // local_blocks)
    before = reach_devices * local_blocks
    anomaly = (ensemble - jnp.mean(ensemble, axis=2, keepdims=True)) / jnp.sqrt(
        jnp.float32(members - 1)
    )
    positions = before + jnp.arange(local_blocks, dtype=jnp.int32)[:, None] - pred_back
    positions = jnp.where(pred_back > 0, positions, before + local_blocks)
    empty_zero_matrix = jnp.zeros((1, rows, members), jnp.float32)

    def extend(entry_values):
        return jnp.concatenate(
            [previous_blocks(entry_values, reach_devices), entry_values, empty_zero_matrix], axis=0
        )

    preds = extend(anomaly)[positions]
    identity = jnp.eye(slots, dtype=jnp.float32)
    gram = jnp.einsum("bjrm,bkrm->jkbr", preds, preds, precision=highest)
    gram = gram + ridge[None, None, :, None] * identity[:, :, None, None]
    target = jnp.einsum("bjrm,brm->jbr", preds, anomaly, precision=highest)
    regression_coefficients = small_solve(gram, target)
    resid = anomaly - jnp.einsum("jbr,bjrm->brm", regression_coefficients, preds, precision=highest)
    inverse_var = 1.0 / (jnp.sum(resid * resid, axis=2) + 1e-05)
    inverse_obs = 1.0 / obs_var
    beta_blocks = jnp.transpose(regression_coefficients, (1, 0, 2))
    lower_bound = bounds[0]
    upper_bound = bounds[1]
    theta = (upper_bound + lower_bound) / 2
    delta = (upper_bound - lower_bound) / 2
    sigma = theta / delta
    rho_now = 1.0 / sigma
    residue = inverse_obs[:, :, None] * (observed - ensemble)
    increment = jnp.zeros_like(ensemble)
    direction = residue / theta
    for step in range(ITERS):
        increment = increment + direction
        extended = extend(direction)
        lower_analysis_output = direction
        for lower_slot in range(slots):
            lower_analysis_output = (
                lower_analysis_output
                - beta_blocks[:, lower_slot, :, None] * extended[positions[:, lower_slot]]
            )
        upper_entry_values = lower_analysis_output * inverse_var[:, :, None]
        window = jnp.zeros((before + local_blocks + 1, rows, members), jnp.float32)
        for slot in range(slots):
            window = window.at[positions[:, slot]].add(
                beta_blocks[:, slot, :, None] * upper_entry_values
            )
        analysis_output = upper_entry_values - window[before : before + local_blocks]
        for shift_by in range(1, reach_devices + 1):
            start = (reach_devices - shift_by) * local_blocks
            analysis_output = analysis_output - from_behind(
                window[start : start + local_blocks], ("region", "blk"), -shift_by
            )
        residue = residue - (analysis_output + inverse_obs[:, :, None] * direction)
        rho_next = 1.0 / (2 * sigma - rho_now)
        direction = rho_next * rho_now * direction + 2 * rho_next / delta * residue
        rho_now = rho_next
    increment = increment + direction
    return ensemble + increment


VMEM_GRANT = 48_000_000
SUB = 8
HALF = SUB // 2
LANES = 128
PLANES = 4
MESH_ID = pl.DeviceIdType.MESH
HIGHEST = lax.Precision.HIGHEST


def place():
    per = lax.axis_size("blk")
    region, blk = lax.axis_index("region"), lax.axis_index("blk")
    return lax.axis_size("region"), per, region, blk, region * per + blk


def peer(where, up, j):
    regions, per, region, blk, unused = where
    depth = per // PLANES
    plane = lax.rem(blk // depth + up, PLANES)
    at = lax.rem(region * depth + lax.rem(blk, depth) + j, regions * depth)
    to, blk_to = at // depth, plane * depth + lax.rem(at, depth)
    return (to, blk_to), to * per + blk_to


def each_peer(where, visit, before=lambda up: None):
    width = where[0] * where[1] // PLANES
    for up in range(PLANES):
        before(up)

        def step(j, carry, up=up):
            visit(*peer(where, up, j))
            return carry

        lax.fori_loop(0 if up else 1, width, step, 0)


def copy_to(src, dst, send_sem, recv_sem, device):
    return pltpu.make_async_remote_copy(
        src_ref=src,
        dst_ref=dst,
        send_sem=send_sem,
        recv_sem=recv_sem,
        device_id=device,
        device_id_type=MESH_ID,
    )


def tile_at(k):
    return pl.ds(pl.multiple_of(k * SUB, SUB), SUB)


def swap(x):
    return pltpu.roll(x, HALF, 0)


def pair_rows(n, src, dst):
    low = lax.broadcasted_iota(jnp.int32, (SUB, LANES), 0) < HALF
    for k in range(n):
        at = slice(k * SUB, (k + 1) * SUB)
        first, second = src[0, at, :], src[1, at, :]
        dst[0, at, :] = jnp.where(low, first, swap(second))
        dst[1, at, :] = jnp.where(low, swap(first), second)


def fill_pack(rows, obs_var, ridge, pred_back, pack):
    local = pred_back.shape[0]
    lane = lax.broadcasted_iota(jnp.int32, (1, LANES), 1)
    groups = LANES // SUB
    side = LANES // local
    for block in range(local):
        meta = jnp.where(lane == SUB + REACH, ridge[block], 0.0)
        for slot in range(pred_back.shape[1]):
            back = pred_back[block, slot]
            meta = jnp.where((lane == back + (SUB - 1)) & (lane >= SUB), 1.0, meta)
        for part in range(rows // LANES):
            row = obs_var[block : block + 1, part * LANES : (part + 1) * LANES]
            for k in range(groups):
                turned = row if k == 0 else pltpu.roll(row, LANES - SUB * k, 1)
                turned = jnp.where(lane < SUB, turned, meta)
                at = part * groups + k
                if block:
                    turned = jnp.where(lane < side, pack[at], pltpu.roll(turned, side, 1))
                pack[at] = turned


def whole_kernel(
    n, bounds_in, ens_in, obs_in, obs_var_in, ridge_in, pred_back_in, z,
    bounds, ens, obs, obs_var, ridge, pred_back, load_sem,
    pack, obs_s, ens_r, obs_r, pack_r, facts, z_s, z_r, ready, send_sem, recv_sem,
    corr, filt,
):
    where = place()
    me = where[-1]
    local, rows, members = ens.shape
    loads = [
        pltpu.make_async_copy(src, dst, load_sem.at[i])
        for i, (src, dst) in enumerate(
            (
                (ens_in, ens),
                (obs_in, obs),
                (obs_var_in, obs_var),
                (ridge_in, ridge),
                (pred_back_in, pred_back),
                (bounds_in, bounds),
            )
        )
    ]
    for load in loads:
        load.start()
    barrier = pltpu.get_barrier_semaphore()


    def signal(sem, up, j):
        device, unused = peer(where, up, j)
        pl.semaphore_signal(sem, inc=1, device_id=device, device_id_type=MESH_ID)

    width = n // PLANES
    for up in range(PLANES):
        for j in range(0 if up else 1, width): signal(barrier, up, j)
    own = tile_at(me)
    mine = pl.ds(me * local, local)
    pl.semaphore_wait(barrier, n - 1)
    loads[0].wait()

    def plane_ready(up):
        if up:
            pass

    def send_ens(device, k):
        copy_to(
            ens.at[:, tile_at(k), :], ens_r.at[mine], send_sem.at[0], recv_sem.at[0], device
        ).start()

    def send_pack(device, k):
        copy_to(pack.at[k], pack_r.at[me], send_sem.at[1], recv_sem.at[1], device).start()

    def send_half(src, dst, h, which):
        def send(device, k):
            copy_to(
                src.at[h, tile_at(k), :], dst.at[h, own, :], send_sem.at[which], recv_sem.at[which],
                device,
            ).start()

        return send

    each_peer(where, send_ens, plane_ready)
    for load in loads[1:]:
        load.wait()
    fill_pack(rows, obs_var, ridge, pred_back, pack)
    each_peer(where, send_pack)
    pair_rows(n, obs, obs_s)
    each_peer(where, send_half(obs_s, obs_r, 0, 2))
    each_peer(where, send_half(obs_s, obs_r, 1, 3))

    ens_r[mine] = ens[:, own, :]
    pack_r[me] = pack[me]
    obs_r[:, own, :] = obs_s[:, own, :]
    others = pl.ds(0, (n - 1) * SUB)
    whole = (
        ens_r.at[pl.ds(0, (n - 1) * local)],
        pack_r.at[pl.ds(0, n - 1)],
        obs_r.at[0, others, :],
        obs_r.at[1, others, :],
        z_r.at[0, others, :],
        z_r.at[1, others, :],
    )
    regions, per, region, blk, unused = where
    neighbour = (lax.rem(region + 1, regions), blk)

    def arrived(which):
        ref = whole[which]
        copy_to(ref, ref, send_sem.at[which], recv_sem.at[which], neighbour).wait_recv()

    arrived(0)
    make_filters(n * local, arrived, bounds, ens_r, pack_r, facts, corr, filt)
    nb = n * local
    empty = jnp.zeros((nb, members), jnp.float32)
    for h in range(2):
        arrived(2 + h)
        for pair in range(HALF // 2):
            gaps = [
                obs_r[h, pl.ds(r, nb, stride=HALF), :] - ens_r[pl.ds(0, nb), h * HALF + r, :]
                for r in (2 * pair, 2 * pair + 1)
            ]
            columns = []
            for r in range(2):
                column = [empty] * 4
                column[2 * r + h] = gaps[r]
                columns.append(jnp.concatenate(column, axis=0))
            found = dot_split(filt[pair], jnp.concatenate(columns, axis=1), 0)
            for r in range(2):
                z_s[h, pl.ds(2 * pair + r, nb, stride=HALF), :] = found[
                    :, r * members : (r + 1) * members
                ]
        each_peer(where, send_half(z_s, z_r, h, 4 + h))
        z_r[h, own, :] = z_s[h, own, :]
    low = lax.broadcasted_iota(jnp.int32, (SUB, LANES), 0) < HALF
    arrived(4)
    arrived(5)
    for k in range(n):
        at = slice(k * SUB, (k + 1) * SUB)
        first, second = z_r[0, at, :], z_r[1, at, :]
        z[0, at, :] = jnp.where(low, first, swap(second))
        z[1, at, :] = jnp.where(low, swap(first), second)
    for which, ref in enumerate(whole):
        copy_to(ref, ref, send_sem.at[which], recv_sem.at[which], neighbour).wait_send()


def dot(lhs, rhs, left, right):
    return lax.dot_general(
        lhs,
        rhs,
        (((left,), (right,)), ((), ())),
        precision=HIGHEST,
        preferred_element_type=jnp.float32,
    )


def halves_of(x):
    high = x.astype(jnp.bfloat16)
    return high, (x - high.astype(jnp.float32)).astype(jnp.bfloat16)


def dot_split(lhs, rhs, right):
    product = lambda a, b: lax.dot_general(
        a, b, (((1,), (right,)), ((), ())), preferred_element_type=jnp.float32
    )
    rows = lhs.shape[0]
    left_high, left_low = halves_of(lhs)
    right_high, right_low = halves_of(rhs)
    both = product(jnp.concatenate([left_high, left_low], axis=0), right_high)
    return both[:rows] + (both[rows:] + product(left_high, right_low))


def spread(x, on):
    return jnp.where(on, jnp.concatenate([x] * (x.shape[1] // x.shape[0]), axis=0), 0.0)


def make_filters(nb, arrived, bounds, ens, pack, facts, corr, filt):
    members = ens.shape[2]
    tile = (SUB, LANES)
    wide = 2 * LANES
    back = lax.rem(lax.broadcasted_iota(jnp.int32, (nb, LANES), 1), nb) - lax.broadcasted_iota(
        jnp.int32, (nb, LANES), 0
    )
    on = lax.broadcasted_iota(jnp.int32, (wide, wide), 0) // nb == lax.broadcasted_iota(
        jnp.int32, (wide, wide), 1
    ) // nb
    empty = jnp.zeros((nb, members), jnp.float32)
    corr[...] = jnp.zeros(corr.shape, jnp.float32)
    anom = []
    for r in range(HALF):
        sides = []
        for h in range(2):
            x = ens[pl.ds(0, nb), h * HALF + r, :]
            mean = jnp.sum(x, axis=1, keepdims=True) * (1.0 / members)
            sides.append((x - mean) * (1.0 / math.sqrt(members - 1)))
        anom.append(jnp.concatenate(sides, axis=0))
        rhs = jnp.concatenate(
            [
                jnp.concatenate([sides[0], empty], axis=1),
                jnp.concatenate([empty, sides[1]], axis=1),
            ],
            axis=0,
        )
        full = dot(jnp.concatenate(sides, axis=1), rhs, 1, 1)
        for delta in range(REACH + 1):
            corr[delta, r : r + 1, :] = jnp.sum(
                jnp.where(back == delta, full, 0.0), axis=0, keepdims=True
            )

    arrived(1)
    devices = pack.shape[0]
    local = nb // devices
    flat = pack[...].reshape(devices, LANES)
    for block in range(local):
        turned = pltpu.roll(flat, block * (LANES // local), 1) if block else flat
        facts[pl.ds(block, devices, stride=local), :] = turned
    flat = facts[...]
    turned = jnp.concatenate([flat, flat], axis=0).T
    on_lane = lax.broadcasted_iota(jnp.int32, tile, 1)
    obs_rows = jnp.where(on_lane < nb, turned[0:SUB], swap(turned[0:SUB]))
    inverse_obs = 1.0 / obs_rows
    chosen = [
        jnp.broadcast_to(turned[SUB + d : SUB + d + 1], tile) > 0.5 for d in range(REACH)
    ]
    at = SUB + REACH
    ridge = jnp.broadcast_to(turned[at : at + 1], tile)

    factor = {}
    inverse = []
    for j in range(REACH):
        for i in range(j, REACH):
            value = pltpu.roll(corr[i - j], j + 1, 1)
            running = jnp.where(chosen[j], jnp.where(chosen[i], value, 0.0), 0.0)
            if i == j:
                running = running + ridge
            for k in range(j):
                running = running - factor[i, k] * factor[j, k]
            if i == j:
                inverse.append(lax.rsqrt(running))
            else:
                factor[i, j] = running * inverse[j]
    forward = []
    for i in range(REACH):
        running = jnp.where(chosen[i], corr[i + 1], 0.0)
        for k in range(i):
            running = running - factor[i, k] * forward[k]
        forward.append(running * inverse[i])
    beta = [None] * REACH
    for i in reversed(range(REACH)):
        running = forward[i]
        for k in range(i + 1, REACH):
            running = running - factor[k, i] * beta[k]
        beta[i] = running * inverse[i]

    lo = jnp.full((1, wide), bounds[0], jnp.float32)
    hi = jnp.full((1, wide), bounds[1], jnp.float32)
    theta = (hi + lo) / 2
    delta = (hi - lo) / 2
    sigma = theta / delta
    here = back == 0
    identity = jnp.where(jnp.concatenate([here, here], axis=1), 1.0, 0.0)
    pairs = range(HALF // 2)
    rows = lambda pair: (2 * pair, 2 * pair + 1)
    inverse_row = [
        jnp.concatenate([inverse_obs[r : r + 1] for r in rows(pair)], axis=1) for pair in pairs
    ]
    upper = []
    for pair in pairs:
        sides = []
        for r in rows(pair):
            side = jnp.where(here, 1.0, 0.0)
            for d in range(REACH):
                side = jnp.where(back == d + 1, -beta[d][r : r + 1], side)
            sides.append(side)
        upper.append(jnp.concatenate(sides, axis=1))
    spread_upper = [spread(x, on) for x in upper]
    resid = [
        dot(jnp.concatenate([anom[r] for r in rows(pair)], axis=0), spread_upper[pair], 0, 0)
        for pair in pairs
    ]
    inverse_var = [1.0 / (jnp.sum(x * x, axis=0, keepdims=True) + 1e-05) for x in resid]
    operator = [
        dot_split(upper[pair] * inverse_var[pair], spread_upper[pair], 1)
        + identity * inverse_row[pair]
        for pair in pairs
    ]
    spread_operator = [spread(x, on) for x in operator]
    rho = 1.0 / sigma
    direction = [identity / theta for pair in pairs]
    total = direction
    residue = [identity for pair in pairs]
    for step in range(ITERS):
        moved = [
            operator[pair] / theta if step == 0 else dot_split(direction[pair], spread_operator[pair], 0)
            for pair in pairs
        ]
        residue = [residue[pair] - moved[pair] for pair in pairs]
        rho_next = 1.0 / (2 * sigma - rho)
        keep = rho_next * rho
        move = 2 * rho_next / delta
        rho = rho_next
        direction = [keep * direction[pair] + move * residue[pair] for pair in pairs]
        total = [total[pair] + direction[pair] for pair in pairs]
    for pair in pairs:
        filt[pair] = total[pair] * inverse_row[pair]


def by_rows(n, ensemble, observed, obs_var, ridge, pred_back, bounds):
    local, rows, members = ensemble.shape
    nb = n * local
    f32 = jnp.float32
    vmem = pl.BlockSpec(memory_space=pltpu.VMEM)
    hbm = pl.BlockSpec(memory_space=pltpu.HBM)
    halves = pltpu.VMEM((2, n * SUB, members), f32)
    z = pl.pallas_call(
        functools.partial(whole_kernel, n),
        out_shape=pltpu.VMEM(ensemble.shape, f32),
        in_specs=[hbm] * 6,
        out_specs=vmem,
        scratch_shapes=[
            pltpu.SMEM(bounds.shape, f32),
            pltpu.VMEM(ensemble.shape, f32),
            pltpu.VMEM(observed.shape, f32),
            pltpu.VMEM(obs_var.shape, f32),
            pltpu.SMEM(ridge.shape, f32),
            pltpu.SMEM(pred_back.shape, jnp.int32),
            pltpu.SemaphoreType.DMA((6,)),
            pltpu.VMEM((n, 1, LANES), f32),
            halves,
            pltpu.VMEM((nb, SUB, members), f32),
            halves,
            pltpu.VMEM((n, 1, LANES), f32),
            pltpu.VMEM((nb, LANES), f32),
            halves,
            halves,
            pltpu.SemaphoreType.REGULAR((PLANES,)),
            pltpu.SemaphoreType.DMA((6,)),
            pltpu.SemaphoreType.DMA((6,)),
            pltpu.VMEM((REACH + 1, SUB, LANES), f32),
            pltpu.VMEM((HALF // 2, nb, 2 * LANES), f32),
        ],
        compiler_params=pltpu.CompilerParams(
            collective_id=0, has_side_effects=True, vmem_limit_bytes=VMEM_GRANT
        ),
        name="whole",
    )(*[
        pltpu.with_memory_space_constraint(x, pltpu.HBM)
        for x in (bounds, ensemble, observed, obs_var, ridge, pred_back)
    ])
    return ensemble + z


def choose(n, ensemble, *rest):
    local, rows, members = ensemble.shape
    even = lax.axis_size("blk") % PLANES == 0 and local == 2
    if even and rows == n * SUB and members == LANES and 2 * n * local == LANES:
        return by_rows(n, ensemble, *rest)
    return on_device(ensemble, *rest)


def solution(mesh):
    return jax.shard_map(
        functools.partial(choose, mesh.size),
        mesh=mesh,
        in_specs=(
            P(("region", "blk"), None, None),
            P(("region", "blk"), None, None),
            P(("region", "blk"), None),
            P(("region", "blk")),
            P(("region", "blk"), None),
            P(),
        ),
        out_specs=P(("region", "blk"), None, None),
        check_vma=False,
    )
```

```python
import functools
import math

import jax
import jax.numpy as jnp
from jax import lax
from jax.experimental import pallas as pl
from jax.experimental.pallas import tpu as pltpu
from jax.sharding import PartitionSpec as P

REACH = 16
ITERS = 3


def from_behind(value, axis, steps):
    count = lax.axis_size(axis)
    first, last = (max(0, -steps), min(count, count - steps))
    return lax.ppermute(value, axis, [(source, source + steps) for source in range(first, last)])


def small_solve(gram, target):
    size = gram.shape[0]
    factor = {}
    for block_position in range(size):
        running = gram[block_position, block_position]
        for k in range(block_position):
            running = running - factor[block_position, k] * factor[block_position, k]
        factor[block_position, block_position] = jnp.sqrt(running)
        for i in range(block_position + 1, size):
            running = gram[i, block_position]
            for k in range(block_position):
                running = running - factor[i, k] * factor[block_position, k]
            factor[i, block_position] = running / factor[block_position, block_position]
    forward = []
    for i in range(size):
        running = target[i]
        for k in range(i):
            running = running - factor[i, k] * forward[k]
        forward.append(running / factor[i, i])
    analysis_output = [None] * size
    for i in reversed(range(size)):
        running = forward[i]
        for k in range(i + 1, size):
            running = running - factor[k, i] * analysis_output[k]
        analysis_output[i] = running / factor[i, i]
    return jnp.stack(analysis_output)


def previous_blocks(entry_values, reach_devices):
    pieces = [
        from_behind(entry_values, ("region", "blk"), shift_by)
        for shift_by in range(reach_devices, 0, -1)
    ]
    return jnp.concatenate(pieces, axis=0)


def on_device(ensemble, observed, obs_var, ridge, pred_back, bounds):
    highest = lax.Precision.HIGHEST
    local_blocks, rows, members = ensemble.shape
    slots = pred_back.shape[1]
    reach_devices = -(-REACH // local_blocks)
    before = reach_devices * local_blocks
    anomaly = (ensemble - jnp.mean(ensemble, axis=2, keepdims=True)) / jnp.sqrt(
        jnp.float32(members - 1)
    )
    positions = before + jnp.arange(local_blocks, dtype=jnp.int32)[:, None] - pred_back
    positions = jnp.where(pred_back > 0, positions, before + local_blocks)
    empty_zero_matrix = jnp.zeros((1, rows, members), jnp.float32)

    def extend(entry_values):
        return jnp.concatenate(
            [previous_blocks(entry_values, reach_devices), entry_values, empty_zero_matrix], axis=0
        )

    preds = extend(anomaly)[positions]
    identity = jnp.eye(slots, dtype=jnp.float32)
    gram = jnp.einsum("bjrm,bkrm->jkbr", preds, preds, precision=highest)
    gram = gram + ridge[None, None, :, None] * identity[:, :, None, None]
    target = jnp.einsum("bjrm,brm->jbr", preds, anomaly, precision=highest)
    regression_coefficients = small_solve(gram, target)
    resid = anomaly - jnp.einsum("jbr,bjrm->brm", regression_coefficients, preds, precision=highest)
    inverse_var = 1.0 / (jnp.sum(resid * resid, axis=2) + 1e-05)
    inverse_obs = 1.0 / obs_var
    beta_blocks = jnp.transpose(regression_coefficients, (1, 0, 2))
    lower_bound = bounds[0]
    upper_bound = bounds[1]
    theta = (upper_bound + lower_bound) / 2
    delta = (upper_bound - lower_bound) / 2
    sigma = theta / delta
    rho_now = 1.0 / sigma
    residue = inverse_obs[:, :, None] * (observed - ensemble)
    increment = jnp.zeros_like(ensemble)
    direction = residue / theta
    for step in range(ITERS):
        increment = increment + direction
        extended = extend(direction)
        lower_analysis_output = direction
        for lower_slot in range(slots):
            lower_analysis_output = (
                lower_analysis_output
                - beta_blocks[:, lower_slot, :, None] * extended[positions[:, lower_slot]]
            )
        upper_entry_values = lower_analysis_output * inverse_var[:, :, None]
        window = jnp.zeros((before + local_blocks + 1, rows, members), jnp.float32)
        for slot in range(slots):
            window = window.at[positions[:, slot]].add(
                beta_blocks[:, slot, :, None] * upper_entry_values
            )
        analysis_output = upper_entry_values - window[before : before + local_blocks]
        for shift_by in range(1, reach_devices + 1):
            start = (reach_devices - shift_by) * local_blocks
            analysis_output = analysis_output - from_behind(
                window[start : start + local_blocks], ("region", "blk"), -shift_by
            )
        residue = residue - (analysis_output + inverse_obs[:, :, None] * direction)
        rho_next = 1.0 / (2 * sigma - rho_now)
        direction = rho_next * rho_now * direction + 2 * rho_next / delta * residue
        rho_now = rho_next
    increment = increment + direction
    return ensemble + increment


VMEM_GRANT = 48_000_000
SUB = 8
HALF = SUB // 2
LANES = 128
PLANES = 4
PARTS = 1
PART = SUB // PARTS
MESH_ID = pl.DeviceIdType.MESH
HIGHEST = lax.Precision.HIGHEST


def place():
    per = lax.axis_size("blk")
    region, blk = lax.axis_index("region"), lax.axis_index("blk")
    return lax.axis_size("region"), per, region, blk, region * per + blk


def peer(where, up, j):
    regions, per, region, blk, unused = where
    depth = per // PLANES
    plane = lax.rem(blk // depth + up, PLANES)
    at = lax.rem(region * depth + lax.rem(blk, depth) + j, regions * depth)
    to, blk_to = at // depth, plane * depth + lax.rem(at, depth)
    return (to, blk_to), to * per + blk_to


def each_peer(where, visit, before=lambda up: None):
    width = where[0] * where[1] // PLANES
    for up in [1, 2, 3, 0]:

        def step(j, carry, up=up):
            visit(*peer(where, up, j))
            return carry

        lax.fori_loop(0 if up else 1, width, step, 0)


def copy_to(src, dst, send_sem, recv_sem, device):
    return pltpu.make_async_remote_copy(
        src_ref=src,
        dst_ref=dst,
        send_sem=send_sem,
        recv_sem=recv_sem,
        device_id=device,
        device_id_type=MESH_ID,
    )


def part_at(part):
    return pl.ds(part * PART, PART)


def rows_at(k, part):
    return pl.ds(pl.multiple_of(k * SUB + part * PART, PART), PART)


def tile_at(k):
    return pl.ds(pl.multiple_of(k * SUB, SUB), SUB)


def fill_facts(rows, obs_var, ridge, pred_back, ens_s):
    local = pred_back.shape[0]
    lane = lax.broadcasted_iota(jnp.int32, (1, LANES), 1)
    groups = LANES // SUB
    for block in range(local):
        meta = jnp.where(lane == SUB + REACH, ridge[block], 0.0)
        for slot in range(pred_back.shape[1]):
            back = pred_back[block, slot]
            meta = jnp.where((lane == back + (SUB - 1)) & (lane >= SUB), 1.0, meta)
        for part in range(rows // LANES):
            row = obs_var[block : block + 1, part * LANES : (part + 1) * LANES]
            for k in range(groups):
                turned = row if k == 0 else pltpu.roll(row, LANES - SUB * k, 1)
                ens_s[block, part * groups + k, SUB : SUB + 1, :] = jnp.where(
                    lane < SUB, turned, meta
                )


def whole_kernel(
    n, bounds_in, ens_in, obs_in, obs_var_in, ridge_in, pred_back_in, z,
    bounds, ens_s, obs, obs_var, ridge, pred_back, load_sem,
    ens_r, obs_r, z_s, send_sem, recv_sem,
    corr, filt,
):
    where = place()
    me = where[-1]
    local, rows, members = obs.shape
    loads = [
        pltpu.make_async_copy(src, dst, load_sem.at[i])
        for i, (src, dst) in enumerate(
            (
                (ens_in.reshape(local, n, SUB, members), ens_s.at[:, :, pl.ds(0, SUB), :]),
                (obs_in, obs),
                (obs_var_in, obs_var),
                (ridge_in, ridge),
                (pred_back_in, pred_back),
                (bounds_in, bounds),
            )
        )
    ]
    for load in loads:
        load.start()
    barrier = pltpu.get_barrier_semaphore()


    def signal(sem, up, j):
        device, unused = peer(where, up, j)
        pl.semaphore_signal(sem, inc=1, device_id=device, device_id_type=MESH_ID)

    width = n // PLANES
    for up in range(PLANES):
        for j in range(0 if up else 1, width): signal(barrier, up, j)
    own = tile_at(me)
    mine = pl.ds(me * local, local)
    held = pl.ds(0, SUB + 1)
    for load in loads:
        load.wait()
    fill_facts(rows, obs_var, ridge, pred_back, ens_s)
    pl.semaphore_wait(barrier, n - 1)
    def send_ens(device, k):
        copy_to(
            ens_s.at[:, k, held, :], ens_r.at[mine, held, :], send_sem.at[0], recv_sem.at[0], device
        ).start()

    def send_obs(part):
        def send(device, k):
            copy_to(
                obs.at[:, rows_at(k, part), :], obs_r.at[mine, part_at(part), :],
                send_sem.at[1 + part], recv_sem.at[1 + part], device,
            ).start()

        return send

    def send_z(part):
        def send(device, k):
            copy_to(
                z_s.at[pl.ds(k * local, local), part_at(part), :], z.at[:, rows_at(me, part), :],
                send_sem.at[1 + PARTS + part], recv_sem.at[1 + PARTS + part], device,
            ).start()

        return send

    each_peer(where, send_ens)
    for part in range(PARTS):
        each_peer(where, send_obs(part))

    ens_r[mine, held, :] = ens_s[:, me, held, :]
    obs_r[mine] = obs[:, own, :]
    got = pl.ds(0, (n - 1) * local)
    sent = pl.ds(0, (n - 1) * SUB)
    whole = (
        ens_r.at[got, held, :],
        *[obs_r.at[got, part_at(part), :] for part in range(PARTS)],
        *[z_s.at[got, part_at(part), :] for part in range(PARTS)],
    )
    regions, per, region, blk, unused = where
    neighbour = (lax.rem(region + 1, regions), blk)

    def arrived(which):
        ref = whole[which]
        copy_to(ref, ref, send_sem.at[which], recv_sem.at[which], neighbour).wait_recv()

    arrived(0)
    make_filters(n * local, bounds, ens_r, corr, filt)
    nb = n * local
    empty = jnp.zeros((nb, members), jnp.float32)
    for part in range(PARTS):
        arrived(1 + part)
        for r in range(part * PART, (part + 1) * PART, 2):
            h, pair = r // HALF, r % HALF // 2
            columns = []
            for side in range(2):
                column = [empty] * 4
                column[2 * side + h] = obs_r[:, r + side, :] - ens_r[:, r + side, :]
                columns.append(jnp.concatenate(column, axis=0))
            found = dot_split(filt[pair], jnp.concatenate(columns, axis=1), 0)
            for side in range(2):
                z_s[:, r + side, :] = found[:, side * members : (side + 1) * members]
        each_peer(where, send_z(part))
    z[:, own, :] = z_s[mine]
    for part in range(PARTS):
        arrived(1 + PARTS + part)
    for which, ref in enumerate(whole):
        copy_to(ref, ref, send_sem.at[which], recv_sem.at[which], neighbour).wait_send()


def dot(lhs, rhs, left, right):
    return lax.dot_general(
        lhs,
        rhs,
        (((left,), (right,)), ((), ())),
        precision=HIGHEST,
        preferred_element_type=jnp.float32,
    )


def halves_of(x):
    high = x.astype(jnp.bfloat16)
    return high, (x - high.astype(jnp.float32)).astype(jnp.bfloat16)


def dot_split(lhs, rhs, right):
    product = lambda a, b: lax.dot_general(
        a, b, (((1,), (right,)), ((), ())), preferred_element_type=jnp.float32
    )
    rows = lhs.shape[0]
    left_high, left_low = halves_of(lhs)
    right_high, right_low = halves_of(rhs)
    both = product(jnp.concatenate([left_high, left_low], axis=0), right_high)
    return both[:rows] + (both[rows:] + product(left_high, right_low))


def spread(x, on):
    return jnp.where(on, jnp.concatenate([x] * (x.shape[1] // x.shape[0]), axis=0), 0.0)


def make_filters(nb, bounds, ens, corr, filt):
    members = ens.shape[2]
    tile = (SUB, LANES)
    wide = 2 * LANES
    back = lax.rem(lax.broadcasted_iota(jnp.int32, (nb, LANES), 1), nb) - lax.broadcasted_iota(
        jnp.int32, (nb, LANES), 0
    )
    on = lax.broadcasted_iota(jnp.int32, (wide, wide), 0) // nb == lax.broadcasted_iota(
        jnp.int32, (wide, wide), 1
    ) // nb
    empty = jnp.zeros((nb, members), jnp.float32)
    corr[...] = jnp.zeros(corr.shape, jnp.float32)
    anom = []
    for r in range(HALF):
        sides = []
        for h in range(2):
            x = ens[:, h * HALF + r, :]
            mean = jnp.sum(x, axis=1, keepdims=True) * (1.0 / members)
            sides.append((x - mean) * (1.0 / math.sqrt(members - 1)))
        anom.append(jnp.concatenate(sides, axis=0))
        rhs = jnp.concatenate(
            [
                jnp.concatenate([sides[0], empty], axis=1),
                jnp.concatenate([empty, sides[1]], axis=1),
            ],
            axis=0,
        )
        full = dot(jnp.concatenate(sides, axis=1), rhs, 1, 1)
        for delta in range(REACH + 1):
            corr[delta, r : r + 1, :] = jnp.sum(
                jnp.where(back == delta, full, 0.0), axis=0, keepdims=True
            )

    flat = ens[:, SUB, :]
    turned = jnp.concatenate([flat, flat], axis=0).T
    on_lane = lax.broadcasted_iota(jnp.int32, tile, 1)
    obs_rows = jnp.where(on_lane < nb, turned[0:SUB], pltpu.roll(turned[0:SUB], HALF, 0))
    inverse_obs = 1.0 / obs_rows
    chosen = [
        jnp.broadcast_to(turned[SUB + d : SUB + d + 1], tile) > 0.5 for d in range(REACH)
    ]
    at = SUB + REACH
    ridge = jnp.broadcast_to(turned[at : at + 1], tile)

    factor = {}
    inverse = []
    for j in range(REACH):
        for i in range(j, REACH):
            value = pltpu.roll(corr[i - j], j + 1, 1)
            running = jnp.where(chosen[j], jnp.where(chosen[i], value, 0.0), 0.0)
            if i == j:
                running = running + ridge
            for k in range(j):
                running = running - factor[i, k] * factor[j, k]
            if i == j:
                inverse.append(lax.rsqrt(running))
            else:
                factor[i, j] = running * inverse[j]
    forward = []
    for i in range(REACH):
        running = jnp.where(chosen[i], corr[i + 1], 0.0)
        for k in range(i):
            running = running - factor[i, k] * forward[k]
        forward.append(running * inverse[i])
    beta = [None] * REACH
    for i in reversed(range(REACH)):
        running = forward[i]
        for k in range(i + 1, REACH):
            running = running - factor[k, i] * beta[k]
        beta[i] = running * inverse[i]

    lo = jnp.full((1, wide), bounds[0], jnp.float32)
    hi = jnp.full((1, wide), bounds[1], jnp.float32)
    theta = (hi + lo) / 2
    delta = (hi - lo) / 2
    sigma = theta / delta
    here = back == 0
    identity = jnp.where(jnp.concatenate([here, here], axis=1), 1.0, 0.0)
    pairs = range(HALF // 2)
    rows = lambda pair: (2 * pair, 2 * pair + 1)
    inverse_row = [
        jnp.concatenate([inverse_obs[r : r + 1] for r in rows(pair)], axis=1) for pair in pairs
    ]
    upper = []
    for pair in pairs:
        sides = []
        for r in rows(pair):
            side = jnp.where(here, 1.0, 0.0)
            for d in range(REACH):
                side = jnp.where(back == d + 1, -beta[d][r : r + 1], side)
            sides.append(side)
        upper.append(jnp.concatenate(sides, axis=1))
    spread_upper = [spread(x, on) for x in upper]
    resid = [
        dot(jnp.concatenate([anom[r] for r in rows(pair)], axis=0), spread_upper[pair], 0, 0)
        for pair in pairs
    ]
    inverse_var = [1.0 / (jnp.sum(x * x, axis=0, keepdims=True) + 1e-05) for x in resid]
    operator = [
        dot_split(upper[pair] * inverse_var[pair], spread_upper[pair], 1)
        + identity * inverse_row[pair]
        for pair in pairs
    ]
    spread_operator = [spread(x, on) for x in operator]
    rho = 1.0 / sigma
    direction = [identity / theta for pair in pairs]
    total = direction
    residue = [identity for pair in pairs]
    for step in range(ITERS):
        moved = [
            operator[pair] / theta if step == 0 else dot_split(direction[pair], spread_operator[pair], 0)
            for pair in pairs
        ]
        residue = [residue[pair] - moved[pair] for pair in pairs]
        rho_next = 1.0 / (2 * sigma - rho)
        keep = rho_next * rho
        move = 2 * rho_next / delta
        rho = rho_next
        direction = [keep * direction[pair] + move * residue[pair] for pair in pairs]
        total = [total[pair] + direction[pair] for pair in pairs]
    for pair in pairs:
        filt[pair] = total[pair] * inverse_row[pair]


def by_rows(n, ensemble, observed, obs_var, ridge, pred_back, bounds):
    local, rows, members = ensemble.shape
    nb = n * local
    f32 = jnp.float32
    vmem = pl.BlockSpec(memory_space=pltpu.VMEM)
    hbm = pl.BlockSpec(memory_space=pltpu.HBM)
    by_block = pltpu.VMEM((nb, SUB, members), f32)
    z = pl.pallas_call(
        functools.partial(whole_kernel, n),
        out_shape=pltpu.VMEM(ensemble.shape, f32),
        in_specs=[hbm] * 6,
        out_specs=vmem,
        scratch_shapes=[
            pltpu.SMEM(bounds.shape, f32),
            pltpu.VMEM((local, n, 2 * SUB, members), f32),
            pltpu.VMEM(observed.shape, f32),
            pltpu.VMEM(obs_var.shape, f32),
            pltpu.SMEM(ridge.shape, f32),
            pltpu.SMEM(pred_back.shape, jnp.int32),
            pltpu.SemaphoreType.DMA((6,)),
            pltpu.VMEM((nb, 2 * SUB, members), f32),
            by_block,
            by_block,
            pltpu.SemaphoreType.DMA((1 + 2 * PARTS,)),
            pltpu.SemaphoreType.DMA((1 + 2 * PARTS,)),
            pltpu.VMEM((REACH + 1, SUB, LANES), f32),
            pltpu.VMEM((HALF // 2, nb, 2 * LANES), f32),
        ],
        compiler_params=pltpu.CompilerParams(
            collective_id=0, has_side_effects=True, vmem_limit_bytes=VMEM_GRANT
        ),
        name="whole",
    )(*[
        pltpu.with_memory_space_constraint(x, pltpu.HBM)
        for x in (bounds, ensemble, observed, obs_var, ridge, pred_back)
    ])
    return ensemble + z


def choose(n, ensemble, *rest):
    local, rows, members = ensemble.shape
    even = lax.axis_size("blk") % PLANES == 0 and local == 2
    if even and rows == n * SUB and members == LANES and 2 * n * local == LANES:
        return by_rows(n, ensemble, *rest)
    return on_device(ensemble, *rest)


def solution(mesh):
    return jax.shard_map(
        functools.partial(choose, mesh.size),
        mesh=mesh,
        in_specs=(
            P(("region", "blk"), None, None),
            P(("region", "blk"), None, None),
            P(("region", "blk"), None),
            P(("region", "blk")),
            P(("region", "blk"), None),
            P(),
        ),
        out_specs=P(("region", "blk"), None, None),
        check_vma=False,
    )
```

```python
import functools
import math

import jax
import jax.numpy as jnp
from jax import lax
from jax.experimental import pallas as pl
from jax.experimental.pallas import tpu as pltpu
from jax.sharding import PartitionSpec as P

REACH = 16
ITERS = 3


def from_behind(value, axis, steps):
    count = lax.axis_size(axis)
    first, last = (max(0, -steps), min(count, count - steps))
    return lax.ppermute(value, axis, [(source, source + steps) for source in range(first, last)])


def small_solve(gram, target):
    size = gram.shape[0]
    factor = {}
    for block_position in range(size):
        running = gram[block_position, block_position]
        for k in range(block_position):
            running = running - factor[block_position, k] * factor[block_position, k]
        factor[block_position, block_position] = jnp.sqrt(running)
        for i in range(block_position + 1, size):
            running = gram[i, block_position]
            for k in range(block_position):
                running = running - factor[i, k] * factor[block_position, k]
            factor[i, block_position] = running / factor[block_position, block_position]
    forward = []
    for i in range(size):
        running = target[i]
        for k in range(i):
            running = running - factor[i, k] * forward[k]
        forward.append(running / factor[i, i])
    analysis_output = [None] * size
    for i in reversed(range(size)):
        running = forward[i]
        for k in range(i + 1, size):
            running = running - factor[k, i] * analysis_output[k]
        analysis_output[i] = running / factor[i, i]
    return jnp.stack(analysis_output)


def previous_blocks(entry_values, reach_devices):
    pieces = [
        from_behind(entry_values, ("region", "blk"), shift_by)
        for shift_by in range(reach_devices, 0, -1)
    ]
    return jnp.concatenate(pieces, axis=0)


def on_device(ensemble, observed, obs_var, ridge, pred_back, bounds):
    highest = lax.Precision.HIGHEST
    local_blocks, rows, members = ensemble.shape
    slots = pred_back.shape[1]
    reach_devices = -(-REACH // local_blocks)
    before = reach_devices * local_blocks
    anomaly = (ensemble - jnp.mean(ensemble, axis=2, keepdims=True)) / jnp.sqrt(
        jnp.float32(members - 1)
    )
    positions = before + jnp.arange(local_blocks, dtype=jnp.int32)[:, None] - pred_back
    positions = jnp.where(pred_back > 0, positions, before + local_blocks)
    empty_zero_matrix = jnp.zeros((1, rows, members), jnp.float32)

    def extend(entry_values):
        return jnp.concatenate(
            [previous_blocks(entry_values, reach_devices), entry_values, empty_zero_matrix], axis=0
        )

    preds = extend(anomaly)[positions]
    identity = jnp.eye(slots, dtype=jnp.float32)
    gram = jnp.einsum("bjrm,bkrm->jkbr", preds, preds, precision=highest)
    gram = gram + ridge[None, None, :, None] * identity[:, :, None, None]
    target = jnp.einsum("bjrm,brm->jbr", preds, anomaly, precision=highest)
    regression_coefficients = small_solve(gram, target)
    resid = anomaly - jnp.einsum("jbr,bjrm->brm", regression_coefficients, preds, precision=highest)
    inverse_var = 1.0 / (jnp.sum(resid * resid, axis=2) + 1e-05)
    inverse_obs = 1.0 / obs_var
    beta_blocks = jnp.transpose(regression_coefficients, (1, 0, 2))
    lower_bound = bounds[0]
    upper_bound = bounds[1]
    theta = (upper_bound + lower_bound) / 2
    delta = (upper_bound - lower_bound) / 2
    sigma = theta / delta
    rho_now = 1.0 / sigma
    residue = inverse_obs[:, :, None] * (observed - ensemble)
    increment = jnp.zeros_like(ensemble)
    direction = residue / theta
    for step in range(ITERS):
        increment = increment + direction
        extended = extend(direction)
        lower_analysis_output = direction
        for lower_slot in range(slots):
            lower_analysis_output = (
                lower_analysis_output
                - beta_blocks[:, lower_slot, :, None] * extended[positions[:, lower_slot]]
            )
        upper_entry_values = lower_analysis_output * inverse_var[:, :, None]
        window = jnp.zeros((before + local_blocks + 1, rows, members), jnp.float32)
        for slot in range(slots):
            window = window.at[positions[:, slot]].add(
                beta_blocks[:, slot, :, None] * upper_entry_values
            )
        analysis_output = upper_entry_values - window[before : before + local_blocks]
        for shift_by in range(1, reach_devices + 1):
            start = (reach_devices - shift_by) * local_blocks
            analysis_output = analysis_output - from_behind(
                window[start : start + local_blocks], ("region", "blk"), -shift_by
            )
        residue = residue - (analysis_output + inverse_obs[:, :, None] * direction)
        rho_next = 1.0 / (2 * sigma - rho_now)
        direction = rho_next * rho_now * direction + 2 * rho_next / delta * residue
        rho_now = rho_next
    increment = increment + direction
    return ensemble + increment


VMEM_GRANT = 48_000_000
SUB = 8
HALF = SUB // 2
LANES = 128
PLANES = 4
PARTS = 1
EARLY = 2
SIGNALS = ((0, 1, 2, 3), (1, 2, 3, 0), (2, 3, 0, 1), (3, 0, 1, 2))
ROUND = ((1, 2, 3, 0), (2, 3, 0, 1), (3, 0, 1, 2), (0, 1, 2, 3))
BACK = ((1, 2, 3, 0), (2, 3, 0, 1), (0, 1, 3, 2), (0, 1, 2, 3))
PART = SUB // PARTS
MESH_ID = pl.DeviceIdType.MESH
HIGHEST = lax.Precision.HIGHEST


def place():
    per = lax.axis_size("blk")
    region, blk = lax.axis_index("region"), lax.axis_index("blk")
    return lax.axis_size("region"), per, region, blk, region * per + blk


def peer(where, plane, j):
    regions, per, region, blk, unused = where
    depth = per // PLANES
    at = lax.rem(region * depth + lax.rem(blk, depth) + j, regions * depth)
    return at, (at // depth, plane * depth + lax.rem(at, depth))


def each_peer(where, visit, order, early=0):
    regions, per, region, blk, me = where
    depth = per // PLANES
    mine = blk // depth
    for plane in range(PLANES):
        for place in range(early):
            k = plane * depth + place

            @pl.when(me != k)
            def ahead(k=k):
                visit((jnp.int32(0), jnp.int32(k)), jnp.int32(k))

    for turn in range(PLANES):
        plane = order[-1][turn]
        for z in range(PLANES - 1):
            plane = jnp.where(mine == z, order[z][turn], plane)

        def step(j, carry, plane=plane):
            at, device = peer(where, plane, j)

            @pl.when(at >= early)
            def later():
                visit(device, device[0] * per + device[1])

            return carry

        lax.fori_loop(jnp.where(plane == mine, 1, 0), regions * depth, step, 0)


def copy_to(src, dst, send_sem, recv_sem, device):
    return pltpu.make_async_remote_copy(
        src_ref=src,
        dst_ref=dst,
        send_sem=send_sem,
        recv_sem=recv_sem,
        device_id=device,
        device_id_type=MESH_ID,
    )


def part_at(part):
    return pl.ds(part * PART, PART)


def rows_at(k, part):
    return pl.ds(pl.multiple_of(k * SUB + part * PART, PART), PART)


def tile_at(k):
    return pl.ds(pl.multiple_of(k * SUB, SUB), SUB)


def fill_facts(rows, obs_var, ridge, pred_back, ens_s):
    local = pred_back.shape[0]
    lane = lax.broadcasted_iota(jnp.int32, (1, LANES), 1)
    groups = LANES // SUB
    for block in range(local):
        meta = jnp.where(lane == SUB + REACH, ridge[block], 0.0)
        for slot in range(pred_back.shape[1]):
            back = pred_back[block, slot]
            meta = jnp.where((lane == back + (SUB - 1)) & (lane >= SUB), 1.0, meta)
        for part in range(rows // LANES):
            row = obs_var[block : block + 1, part * LANES : (part + 1) * LANES]
            for k in range(groups):
                turned = row if k == 0 else pltpu.roll(row, LANES - SUB * k, 1)
                ens_s[block, part * groups + k, SUB : SUB + 1, :] = jnp.where(
                    lane < SUB, turned, meta
                )


def whole_kernel(
    n, bounds_in, ens_in, obs_in, obs_var_in, ridge_in, pred_back_in, z,
    bounds, ens_s, obs, obs_var, ridge, pred_back, load_sem,
    ens_r, obs_r, z_s, send_sem, recv_sem,
    corr, filt,
):
    where = place()
    me = where[-1]
    local, rows, members = obs.shape
    loads = [
        pltpu.make_async_copy(src, dst, load_sem.at[i])
        for i, (src, dst) in enumerate(
            (
                (ens_in.reshape(local, n, SUB, members), ens_s.at[:, :, pl.ds(0, SUB), :]),
                (obs_in, obs),
                (obs_var_in, obs_var),
                (ridge_in, ridge),
                (pred_back_in, pred_back),
                (bounds_in, bounds),
            )
        )
    ]
    for load in loads:
        load.start()
    barrier = pltpu.get_barrier_semaphore()


    def signal(device, k):
        pl.semaphore_signal(barrier, inc=1, device_id=device, device_id_type=MESH_ID)

    each_peer(where, signal, SIGNALS, EARLY)
    own = tile_at(me)
    mine = pl.ds(me * local, local)
    held = pl.ds(0, SUB + 1)
    for load in loads:
        load.wait()
    fill_facts(rows, obs_var, ridge, pred_back, ens_s)
    pl.semaphore_wait(barrier, n - 1)

    def send_ens(device, k):
        copy_to(
            ens_s.at[:, k, held, :], ens_r.at[mine, held, :], send_sem.at[0], recv_sem.at[0], device
        ).start()

    def send_obs(part):
        def send(device, k):
            copy_to(
                obs.at[:, rows_at(k, part), :], obs_r.at[mine, part_at(part), :],
                send_sem.at[1 + part], recv_sem.at[1 + part], device,
            ).start()

        return send

    def send_z(part):
        def send(device, k):
            copy_to(
                z_s.at[pl.ds(k * local, local), part_at(part), :], z.at[:, rows_at(me, part), :],
                send_sem.at[1 + PARTS + part], recv_sem.at[1 + PARTS + part], device,
            ).start()

        return send

    each_peer(where, send_ens, ROUND)
    for part in range(PARTS):
        each_peer(where, send_obs(part), ROUND)
    ens_r[mine, held, :] = ens_s[:, me, held, :]
    obs_r[mine] = obs[:, own, :]
    got = pl.ds(0, (n - 1) * local)
    whole = (
        ens_r.at[got, held, :],
        *[obs_r.at[got, part_at(part), :] for part in range(PARTS)],
        *[z_s.at[got, part_at(part), :] for part in range(PARTS)],
    )
    regions, per, region, blk, unused = where
    neighbour = (lax.rem(region + 1, regions), blk)

    def arrived(which):
        ref = whole[which]
        copy_to(ref, ref, send_sem.at[which], recv_sem.at[which], neighbour).wait_recv()

    arrived(0)
    make_filters(n * local, bounds, ens_r, corr, filt)
    nb = n * local
    empty = jnp.zeros((nb, members), jnp.float32)
    for part in range(PARTS):
        arrived(1 + part)
        for r in range(part * PART, (part + 1) * PART, 2):
            h, pair = r // HALF, r % HALF // 2
            columns = []
            for side in range(2):
                column = [empty] * 4
                column[2 * side + h] = obs_r[:, r + side, :] - ens_r[:, r + side, :]
                columns.append(jnp.concatenate(column, axis=0))
            found = dot_split(filt[pair], jnp.concatenate(columns, axis=1), 0)
            for side in range(2):
                z_s[:, r + side, :] = found[:, side * members : (side + 1) * members]
        each_peer(where, send_z(part), BACK, EARLY)
    z[:, own, :] = z_s[mine]
    for part in range(PARTS):
        arrived(1 + PARTS + part)
    for which, ref in enumerate(whole):
        copy_to(ref, ref, send_sem.at[which], recv_sem.at[which], neighbour).wait_send()


def dot(lhs, rhs, left, right):
    return lax.dot_general(
        lhs,
        rhs,
        (((left,), (right,)), ((), ())),
        precision=HIGHEST,
        preferred_element_type=jnp.float32,
    )


def halves_of(x):
    high = x.astype(jnp.bfloat16)
    return high, (x - high.astype(jnp.float32)).astype(jnp.bfloat16)


def dot_split(lhs, rhs, right):
    product = lambda a, b: lax.dot_general(
        a, b, (((1,), (right,)), ((), ())), preferred_element_type=jnp.float32
    )
    rows = lhs.shape[0]
    left_high, left_low = halves_of(lhs)
    right_high, right_low = halves_of(rhs)
    both = product(jnp.concatenate([left_high, left_low], axis=0), right_high)
    return both[:rows] + (both[rows:] + product(left_high, right_low))


def spread(x, on):
    return jnp.where(on, jnp.concatenate([x] * (x.shape[1] // x.shape[0]), axis=0), 0.0)


def make_filters(nb, bounds, ens, corr, filt):
    members = ens.shape[2]
    tile = (SUB, LANES)
    wide = 2 * LANES
    back = lax.rem(lax.broadcasted_iota(jnp.int32, (nb, LANES), 1), nb) - lax.broadcasted_iota(
        jnp.int32, (nb, LANES), 0
    )
    on = lax.broadcasted_iota(jnp.int32, (wide, wide), 0) // nb == lax.broadcasted_iota(
        jnp.int32, (wide, wide), 1
    ) // nb
    empty = jnp.zeros((nb, members), jnp.float32)
    corr[...] = jnp.zeros(corr.shape, jnp.float32)
    anom = []
    for r in range(HALF):
        sides = []
        for h in range(2):
            x = ens[:, h * HALF + r, :]
            mean = jnp.sum(x, axis=1, keepdims=True) * (1.0 / members)
            sides.append((x - mean) * (1.0 / math.sqrt(members - 1)))
        anom.append(jnp.concatenate(sides, axis=0))
        rhs = jnp.concatenate(
            [
                jnp.concatenate([sides[0], empty], axis=1),
                jnp.concatenate([empty, sides[1]], axis=1),
            ],
            axis=0,
        )
        full = dot(jnp.concatenate(sides, axis=1), rhs, 1, 1)
        for delta in range(REACH + 1):
            corr[delta, r : r + 1, :] = jnp.sum(
                jnp.where(back == delta, full, 0.0), axis=0, keepdims=True
            )

    flat = ens[:, SUB, :]
    turned = jnp.concatenate([flat, flat], axis=0).T
    on_lane = lax.broadcasted_iota(jnp.int32, tile, 1)
    obs_rows = jnp.where(on_lane < nb, turned[0:SUB], pltpu.roll(turned[0:SUB], HALF, 0))
    inverse_obs = 1.0 / obs_rows
    chosen = [
        jnp.broadcast_to(turned[SUB + d : SUB + d + 1], tile) > 0.5 for d in range(REACH)
    ]
    at = SUB + REACH
    ridge = jnp.broadcast_to(turned[at : at + 1], tile)

    factor = {}
    inverse = []
    for j in range(REACH):
        for i in range(j, REACH):
            value = pltpu.roll(corr[i - j], j + 1, 1)
            running = jnp.where(chosen[j], jnp.where(chosen[i], value, 0.0), 0.0)
            if i == j:
                running = running + ridge
            for k in range(j):
                running = running - factor[i, k] * factor[j, k]
            if i == j:
                inverse.append(lax.rsqrt(running))
            else:
                factor[i, j] = running * inverse[j]
    forward = []
    for i in range(REACH):
        running = jnp.where(chosen[i], corr[i + 1], 0.0)
        for k in range(i):
            running = running - factor[i, k] * forward[k]
        forward.append(running * inverse[i])
    beta = [None] * REACH
    for i in reversed(range(REACH)):
        running = forward[i]
        for k in range(i + 1, REACH):
            running = running - factor[k, i] * beta[k]
        beta[i] = running * inverse[i]

    lo = jnp.full((1, wide), bounds[0], jnp.float32)
    hi = jnp.full((1, wide), bounds[1], jnp.float32)
    theta = (hi + lo) / 2
    delta = (hi - lo) / 2
    sigma = theta / delta
    here = back == 0
    identity = jnp.where(jnp.concatenate([here, here], axis=1), 1.0, 0.0)
    pairs = range(HALF // 2)
    rows = lambda pair: (2 * pair, 2 * pair + 1)
    inverse_row = [
        jnp.concatenate([inverse_obs[r : r + 1] for r in rows(pair)], axis=1) for pair in pairs
    ]
    upper = []
    for pair in pairs:
        sides = []
        for r in rows(pair):
            side = jnp.where(here, 1.0, 0.0)
            for d in range(REACH):
                side = jnp.where(back == d + 1, -beta[d][r : r + 1], side)
            sides.append(side)
        upper.append(jnp.concatenate(sides, axis=1))
    spread_upper = [spread(x, on) for x in upper]
    resid = [
        dot(jnp.concatenate([anom[r] for r in rows(pair)], axis=0), spread_upper[pair], 0, 0)
        for pair in pairs
    ]
    inverse_var = [1.0 / (jnp.sum(x * x, axis=0, keepdims=True) + 1e-05) for x in resid]
    operator = [
        dot_split(upper[pair] * inverse_var[pair], spread_upper[pair], 1)
        + identity * inverse_row[pair]
        for pair in pairs
    ]
    spread_operator = [spread(x, on) for x in operator]
    rho = 1.0 / sigma
    direction = [identity / theta for pair in pairs]
    total = direction
    residue = [identity for pair in pairs]
    for step in range(ITERS):
        moved = [
            operator[pair] / theta if step == 0 else dot_split(direction[pair], spread_operator[pair], 0)
            for pair in pairs
        ]
        residue = [residue[pair] - moved[pair] for pair in pairs]
        rho_next = 1.0 / (2 * sigma - rho)
        keep = rho_next * rho
        move = 2 * rho_next / delta
        rho = rho_next
        direction = [keep * direction[pair] + move * residue[pair] for pair in pairs]
        total = [total[pair] + direction[pair] for pair in pairs]
    for pair in pairs:
        filt[pair] = total[pair] * inverse_row[pair]


def by_rows(n, ensemble, observed, obs_var, ridge, pred_back, bounds):
    local, rows, members = ensemble.shape
    nb = n * local
    f32 = jnp.float32
    vmem = pl.BlockSpec(memory_space=pltpu.VMEM)
    hbm = pl.BlockSpec(memory_space=pltpu.HBM)
    by_block = pltpu.VMEM((nb, SUB, members), f32)
    z = pl.pallas_call(
        functools.partial(whole_kernel, n),
        out_shape=pltpu.VMEM(ensemble.shape, f32),
        in_specs=[hbm] * 6,
        out_specs=vmem,
        scratch_shapes=[
            pltpu.SMEM(bounds.shape, f32),
            pltpu.VMEM((local, n, 2 * SUB, members), f32),
            pltpu.VMEM(observed.shape, f32),
            pltpu.VMEM(obs_var.shape, f32),
            pltpu.SMEM(ridge.shape, f32),
            pltpu.SMEM(pred_back.shape, jnp.int32),
            pltpu.SemaphoreType.DMA((6,)),
            pltpu.VMEM((nb, 2 * SUB, members), f32),
            by_block,
            by_block,
            pltpu.SemaphoreType.DMA((1 + 2 * PARTS,)),
            pltpu.SemaphoreType.DMA((1 + 2 * PARTS,)),
            pltpu.VMEM((REACH + 1, SUB, LANES), f32),
            pltpu.VMEM((HALF // 2, nb, 2 * LANES), f32),
        ],
        compiler_params=pltpu.CompilerParams(
            collective_id=0, has_side_effects=True, vmem_limit_bytes=VMEM_GRANT
        ),
        name="whole",
    )(*[
        pltpu.with_memory_space_constraint(x, pltpu.HBM)
        for x in (bounds, ensemble, observed, obs_var, ridge, pred_back)
    ])
    return ensemble + z


def choose(n, ensemble, *rest):
    local, rows, members = ensemble.shape
    even = lax.axis_size("blk") % PLANES == 0 and local == 2
    if even and rows == n * SUB and members == LANES and 2 * n * local == LANES:
        return by_rows(n, ensemble, *rest)
    return on_device(ensemble, *rest)


def solution(mesh):
    return jax.shard_map(
        functools.partial(choose, mesh.size),
        mesh=mesh,
        in_specs=(
            P(("region", "blk"), None, None),
            P(("region", "blk"), None, None),
            P(("region", "blk"), None),
            P(("region", "blk")),
            P(("region", "blk"), None),
            P(),
        ),
        out_specs=P(("region", "blk"), None, None),
        check_vma=False,
    )
```

```python
import functools
import math

import jax
import jax.numpy as jnp
from jax import lax
from jax.experimental import pallas as pl
from jax.experimental.pallas import tpu as pltpu
from jax.sharding import PartitionSpec as P

REACH = 16
ITERS = 3


def from_behind(value, axis, steps):
    count = lax.axis_size(axis)
    first, last = (max(0, -steps), min(count, count - steps))
    return lax.ppermute(value, axis, [(source, source + steps) for source in range(first, last)])


def small_solve(gram, target):
    size = gram.shape[0]
    factor = {}
    for block_position in range(size):
        running = gram[block_position, block_position]
        for k in range(block_position):
            running = running - factor[block_position, k] * factor[block_position, k]
        factor[block_position, block_position] = jnp.sqrt(running)
        for i in range(block_position + 1, size):
            running = gram[i, block_position]
            for k in range(block_position):
                running = running - factor[i, k] * factor[block_position, k]
            factor[i, block_position] = running / factor[block_position, block_position]
    forward = []
    for i in range(size):
        running = target[i]
        for k in range(i):
            running = running - factor[i, k] * forward[k]
        forward.append(running / factor[i, i])
    analysis_output = [None] * size
    for i in reversed(range(size)):
        running = forward[i]
        for k in range(i + 1, size):
            running = running - factor[k, i] * analysis_output[k]
        analysis_output[i] = running / factor[i, i]
    return jnp.stack(analysis_output)


def previous_blocks(entry_values, reach_devices):
    pieces = [
        from_behind(entry_values, ("region", "blk"), shift_by)
        for shift_by in range(reach_devices, 0, -1)
    ]
    return jnp.concatenate(pieces, axis=0)


def on_device(ensemble, observed, obs_var, ridge, pred_back, bounds):
    highest = lax.Precision.HIGHEST
    local_blocks, rows, members = ensemble.shape
    slots = pred_back.shape[1]
    reach_devices = -(-REACH // local_blocks)
    before = reach_devices * local_blocks
    anomaly = (ensemble - jnp.mean(ensemble, axis=2, keepdims=True)) / jnp.sqrt(
        jnp.float32(members - 1)
    )
    positions = before + jnp.arange(local_blocks, dtype=jnp.int32)[:, None] - pred_back
    positions = jnp.where(pred_back > 0, positions, before + local_blocks)
    empty_zero_matrix = jnp.zeros((1, rows, members), jnp.float32)

    def extend(entry_values):
        return jnp.concatenate(
            [previous_blocks(entry_values, reach_devices), entry_values, empty_zero_matrix], axis=0
        )

    preds = extend(anomaly)[positions]
    identity = jnp.eye(slots, dtype=jnp.float32)
    gram = jnp.einsum("bjrm,bkrm->jkbr", preds, preds, precision=highest)
    gram = gram + ridge[None, None, :, None] * identity[:, :, None, None]
    target = jnp.einsum("bjrm,brm->jbr", preds, anomaly, precision=highest)
    regression_coefficients = small_solve(gram, target)
    resid = anomaly - jnp.einsum("jbr,bjrm->brm", regression_coefficients, preds, precision=highest)
    inverse_var = 1.0 / (jnp.sum(resid * resid, axis=2) + 1e-05)
    inverse_obs = 1.0 / obs_var
    beta_blocks = jnp.transpose(regression_coefficients, (1, 0, 2))
    lower_bound = bounds[0]
    upper_bound = bounds[1]
    theta = (upper_bound + lower_bound) / 2
    delta = (upper_bound - lower_bound) / 2
    sigma = theta / delta
    rho_now = 1.0 / sigma
    residue = inverse_obs[:, :, None] * (observed - ensemble)
    increment = jnp.zeros_like(ensemble)
    direction = residue / theta
    for step in range(ITERS):
        increment = increment + direction
        extended = extend(direction)
        lower_analysis_output = direction
        for lower_slot in range(slots):
            lower_analysis_output = (
                lower_analysis_output
                - beta_blocks[:, lower_slot, :, None] * extended[positions[:, lower_slot]]
            )
        upper_entry_values = lower_analysis_output * inverse_var[:, :, None]
        window = jnp.zeros((before + local_blocks + 1, rows, members), jnp.float32)
        for slot in range(slots):
            window = window.at[positions[:, slot]].add(
                beta_blocks[:, slot, :, None] * upper_entry_values
            )
        analysis_output = upper_entry_values - window[before : before + local_blocks]
        for shift_by in range(1, reach_devices + 1):
            start = (reach_devices - shift_by) * local_blocks
            analysis_output = analysis_output - from_behind(
                window[start : start + local_blocks], ("region", "blk"), -shift_by
            )
        residue = residue - (analysis_output + inverse_obs[:, :, None] * direction)
        rho_next = 1.0 / (2 * sigma - rho_now)
        direction = rho_next * rho_now * direction + 2 * rho_next / delta * residue
        rho_now = rho_next
    increment = increment + direction
    return ensemble + increment


VMEM_GRANT = 48_000_000
SUB = 8
HALF = SUB // 2
LANES = 128
PLANES = 4
PARTS = 1
EARLY = 2
SIGNALS = ((0, 1, 2, 3), (1, 2, 3, 0), (2, 3, 0, 1), (3, 0, 1, 2))
ROUND = ((1, 2, 3, 0), (2, 3, 0, 1), (3, 0, 1, 2), (0, 1, 2, 3))
BACK = ((1, 2, 3, 0), (2, 3, 0, 1), (0, 1, 3, 2), (0, 1, 2, 3))
PART = SUB // PARTS
MESH_ID = pl.DeviceIdType.MESH
HIGHEST = lax.Precision.HIGHEST


def place():
    per = lax.axis_size("blk")
    region, blk = lax.axis_index("region"), lax.axis_index("blk")
    return lax.axis_size("region"), per, region, blk, region * per + blk


def peer(where, plane, j):
    regions, per, region, blk, unused = where
    depth = per // PLANES
    at = lax.rem(region * depth + lax.rem(blk, depth) + j, regions * depth)
    return at, (at // depth, plane * depth + lax.rem(at, depth))


def each_peer(where, visit, order, early=0):
    regions, per, region, blk, me = where
    depth = per // PLANES
    mine = blk // depth
    for plane in range(PLANES):
        for place in range(early):
            k = plane * depth + place

            @pl.when(me != k)
            def ahead(k=k):
                visit((jnp.int32(0), jnp.int32(k)), jnp.int32(k))

    for turn in range(PLANES):
        plane = order[-1][turn]
        for z in range(PLANES - 1):
            plane = jnp.where(mine == z, order[z][turn], plane)

        def step(j, carry, plane=plane):
            at, device = peer(where, plane, j)

            @pl.when(at >= early)
            def later():
                visit(device, device[0] * per + device[1])

            return carry

        lax.fori_loop(jnp.where(plane == mine, 1, 0), regions * depth, step, 0)


def copy_to(src, dst, send_sem, recv_sem, device):
    return pltpu.make_async_remote_copy(
        src_ref=src,
        dst_ref=dst,
        send_sem=send_sem,
        recv_sem=recv_sem,
        device_id=device,
        device_id_type=MESH_ID,
    )


def part_at(part):
    return pl.ds(part * PART, PART)


def rows_at(k, part):
    return pl.ds(pl.multiple_of(k * SUB + part * PART, PART), PART)


def tile_at(k):
    return pl.ds(pl.multiple_of(k * SUB, SUB), SUB)


def fill_facts(rows, obs_var, ridge, pred_back, ens_s):
    local = pred_back.shape[0]
    lane = lax.broadcasted_iota(jnp.int32, (1, LANES), 1)
    groups = LANES // SUB
    for block in range(local):
        meta = jnp.where(lane == SUB + REACH, ridge[block], 0.0)
        for slot in range(pred_back.shape[1]):
            back = pred_back[block, slot]
            meta = jnp.where((lane == back + (SUB - 1)) & (lane >= SUB), 1.0, meta)
        for part in range(rows // LANES):
            row = obs_var[block : block + 1, part * LANES : (part + 1) * LANES]
            for k in range(groups):
                turned = row if k == 0 else pltpu.roll(row, LANES - SUB * k, 1)
                ens_s[block, part * groups + k, SUB : SUB + 1, :] = jnp.where(
                    lane < SUB, turned, meta
                )


def whole_kernel(
    n, bounds_in, ens_in, obs_in, obs_var_in, ridge_in, pred_back_in, z,
    bounds, ens_s, obs, obs_var, ridge, pred_back, load_sem,
    ens_r, obs_r, z_s, send_sem, recv_sem,
    corr, filt,
):
    where = place()
    me = where[-1]
    local, rows, members = obs.shape
    loads = [
        pltpu.make_async_copy(src, dst, load_sem.at[i])
        for i, (src, dst) in enumerate(
            (
                (ens_in.reshape(local, n, SUB, members), ens_s.at[:, :, pl.ds(0, SUB), :]),
                (obs_in, obs),
                (obs_var_in, obs_var),
                (ridge_in, ridge),
                (pred_back_in, pred_back),
                (bounds_in, bounds),
            )
        )
    ]
    for load in loads:
        load.start()
    barrier = pltpu.get_barrier_semaphore()


    def signal(device, k):
        pl.semaphore_signal(barrier, inc=1, device_id=device, device_id_type=MESH_ID)

    each_peer(where, signal, SIGNALS, EARLY)
    own = tile_at(me)
    mine = pl.ds(me * local, local)
    held = pl.ds(0, SUB + 1)
    for load in loads:
        load.wait()
    fill_facts(rows, obs_var, ridge, pred_back, ens_s)
    pl.semaphore_wait(barrier, n - 1)

    def send_ens(device, k):
        copy_to(
            ens_s.at[:, k, held, :], ens_r.at[mine, held, :], send_sem.at[0], recv_sem.at[0], device
        ).start()

    def send_obs(part):
        def send(device, k):
            copy_to(
                obs.at[:, rows_at(k, part), :], obs_r.at[mine, part_at(part), :],
                send_sem.at[1 + part], recv_sem.at[1 + part], device,
            ).start()

        return send

    def send_z(part):
        def send(device, k):
            copy_to(
                z_s.at[pl.ds(k * local, local), part_at(part), :], z.at[:, rows_at(me, part), :],
                send_sem.at[1 + PARTS + part], recv_sem.at[1 + PARTS + part], device,
            ).start()

        return send

    each_peer(where, send_ens, ROUND)
    for part in range(PARTS):
        each_peer(where, send_obs(part), ROUND)
    ens_r[mine, held, :] = ens_s[:, me, held, :]
    obs_r[mine] = obs[:, own, :]
    got = pl.ds(0, (n - 1) * local)
    whole = (
        ens_r.at[got, held, :],
        *[obs_r.at[got, part_at(part), :] for part in range(PARTS)],
        *[z_s.at[got, part_at(part), :] for part in range(PARTS)],
    )
    regions, per, region, blk, unused = where
    neighbour = (lax.rem(region + 1, regions), blk)

    def arrived(which):
        ref = whole[which]
        copy_to(ref, ref, send_sem.at[which], recv_sem.at[which], neighbour).wait_recv()

    arrived(0)
    make_filters(n * local, bounds, ens_r, corr, filt)
    nb = n * local
    empty = jnp.zeros((nb, members), jnp.float32)
    for part in range(PARTS):
        arrived(1 + part)
        for r in range(part * PART, (part + 1) * PART, 2):
            h, pair = r // HALF, r % HALF // 2
            columns = []
            for side in range(2):
                column = [empty] * 4
                column[2 * side + h] = obs_r[:, r + side, :] - ens_r[:, r + side, :]
                columns.append(jnp.concatenate(column, axis=0))
            found = dot_split(filt[pair], jnp.concatenate(columns, axis=1), 0)
            for side in range(2):
                z_s[:, r + side, :] = found[:, side * members : (side + 1) * members]
        each_peer(where, send_z(part), BACK, EARLY)
    z[:, own, :] = z_s[mine]
    for part in range(PARTS):
        arrived(1 + PARTS + part)
    for which, ref in enumerate(whole):
        copy_to(ref, ref, send_sem.at[which], recv_sem.at[which], neighbour).wait_send()


def dot(lhs, rhs, left, right):
    return lax.dot_general(
        lhs,
        rhs,
        (((left,), (right,)), ((), ())),
        precision=HIGHEST,
        preferred_element_type=jnp.float32,
    )


def halves_of(x):
    high = x.astype(jnp.bfloat16)
    return high, (x - high.astype(jnp.float32)).astype(jnp.bfloat16)


def dot_split(lhs, rhs, right):
    product = lambda a, b: lax.dot_general(
        a, b, (((1,), (right,)), ((), ())), preferred_element_type=jnp.float32
    )
    if lhs.dtype != jnp.bfloat16:
        lhs = jnp.concatenate(halves_of(lhs), axis=0)
    rows = lhs.shape[0] // 2
    right_high, right_low = halves_of(rhs)
    both = product(lhs, right_high)
    return both[:rows] + (both[rows:] + product(lhs[:rows], right_low))


def spread(x, on):
    return jnp.where(on, jnp.concatenate([x] * (x.shape[1] // x.shape[0]), axis=0), 0.0)


def make_filters(nb, bounds, ens, corr, filt):
    members = ens.shape[2]
    tile = (SUB, LANES)
    wide = 2 * LANES
    back = lax.rem(lax.broadcasted_iota(jnp.int32, (nb, LANES), 1), nb) - lax.broadcasted_iota(
        jnp.int32, (nb, LANES), 0
    )
    on = lax.broadcasted_iota(jnp.int32, (wide, wide), 0) // nb == lax.broadcasted_iota(
        jnp.int32, (wide, wide), 1
    ) // nb
    empty = jnp.zeros((nb, members), jnp.float32)
    corr[...] = jnp.zeros(corr.shape, jnp.float32)
    anom = []
    for r in range(HALF):
        sides = []
        for h in range(2):
            x = ens[:, h * HALF + r, :]
            mean = jnp.sum(x, axis=1, keepdims=True) * (1.0 / members)
            sides.append((x - mean) * (1.0 / math.sqrt(members - 1)))
        anom.append(jnp.concatenate(sides, axis=0))
        rhs = jnp.concatenate(
            [
                jnp.concatenate([sides[0], empty], axis=1),
                jnp.concatenate([empty, sides[1]], axis=1),
            ],
            axis=0,
        )
        full = dot(jnp.concatenate(sides, axis=1), rhs, 1, 1)
        for delta in range(REACH + 1):
            corr[delta, r : r + 1, :] = jnp.sum(
                jnp.where(back == delta, full, 0.0), axis=0, keepdims=True
            )

    flat = ens[:, SUB, :]
    turned = jnp.concatenate([flat, flat], axis=0).T
    on_lane = lax.broadcasted_iota(jnp.int32, tile, 1)
    obs_rows = jnp.where(on_lane < nb, turned[0:SUB], pltpu.roll(turned[0:SUB], HALF, 0))
    inverse_obs = 1.0 / obs_rows
    chosen = [
        jnp.broadcast_to(turned[SUB + d : SUB + d + 1], tile) > 0.5 for d in range(REACH)
    ]
    at = SUB + REACH
    ridge = jnp.broadcast_to(turned[at : at + 1], tile)

    factor = {}
    inverse = []
    for j in range(REACH):
        for i in range(j, REACH):
            value = pltpu.roll(corr[i - j], j + 1, 1)
            running = jnp.where(chosen[j], jnp.where(chosen[i], value, 0.0), 0.0)
            if i == j:
                running = running + ridge
            for k in range(j):
                running = running - factor[i, k] * factor[j, k]
            if i == j:
                inverse.append(lax.rsqrt(running))
            else:
                factor[i, j] = running * inverse[j]
    forward = []
    for i in range(REACH):
        running = jnp.where(chosen[i], corr[i + 1], 0.0)
        for k in range(i):
            running = running - factor[i, k] * forward[k]
        forward.append(running * inverse[i])
    beta = [None] * REACH
    for i in reversed(range(REACH)):
        running = forward[i]
        for k in range(i + 1, REACH):
            running = running - factor[k, i] * beta[k]
        beta[i] = running * inverse[i]

    lo = jnp.full((1, wide), bounds[0], jnp.float32)
    hi = jnp.full((1, wide), bounds[1], jnp.float32)
    theta = (hi + lo) / 2
    delta = (hi - lo) / 2
    sigma = theta / delta
    here = back == 0
    identity = jnp.where(jnp.concatenate([here, here], axis=1), 1.0, 0.0)
    pairs = range(HALF // 2)
    rows = lambda pair: (2 * pair, 2 * pair + 1)
    inverse_row = [
        jnp.concatenate([inverse_obs[r : r + 1] for r in rows(pair)], axis=1) for pair in pairs
    ]
    upper = []
    for pair in pairs:
        sides = []
        for r in rows(pair):
            side = jnp.where(here, 1.0, 0.0)
            for d in range(REACH):
                side = jnp.where(back == d + 1, -beta[d][r : r + 1], side)
            sides.append(side)
        upper.append(jnp.concatenate(sides, axis=1))
    spread_upper = [spread(x, on) for x in upper]
    resid = [
        dot(jnp.concatenate([anom[r] for r in rows(pair)], axis=0), spread_upper[pair], 0, 0)
        for pair in pairs
    ]
    inverse_var = [1.0 / (jnp.sum(x * x, axis=0, keepdims=True) + 1e-05) for x in resid]
    operator = [
        dot_split(upper[pair] * inverse_var[pair], spread_upper[pair], 1)
        + identity * inverse_row[pair]
        for pair in pairs
    ]
    spread_operator = [spread(x, on) for x in operator]
    rho = 1.0 / sigma
    direction = [identity / theta for pair in pairs]
    total = direction
    residue = [identity for pair in pairs]
    for step in range(ITERS):
        moved = [
            operator[pair] / theta if step == 0 else dot_split(direction[pair], spread_operator[pair], 0)
            for pair in pairs
        ]
        residue = [residue[pair] - moved[pair] for pair in pairs]
        rho_next = 1.0 / (2 * sigma - rho)
        keep = rho_next * rho
        move = 2 * rho_next / delta
        rho = rho_next
        direction = [keep * direction[pair] + move * residue[pair] for pair in pairs]
        total = [total[pair] + direction[pair] for pair in pairs]
    for pair in pairs:
        filt[pair] = jnp.concatenate(halves_of(total[pair] * inverse_row[pair]), axis=0)


def by_rows(n, ensemble, observed, obs_var, ridge, pred_back, bounds):
    local, rows, members = ensemble.shape
    nb = n * local
    f32 = jnp.float32
    vmem = pl.BlockSpec(memory_space=pltpu.VMEM)
    hbm = pl.BlockSpec(memory_space=pltpu.HBM)
    by_block = pltpu.VMEM((nb, SUB, members), f32)
    z = pl.pallas_call(
        functools.partial(whole_kernel, n),
        out_shape=pltpu.VMEM(ensemble.shape, f32),
        in_specs=[hbm] * 6,
        out_specs=vmem,
        scratch_shapes=[
            pltpu.SMEM(bounds.shape, f32),
            pltpu.VMEM((local, n, 2 * SUB, members), f32),
            pltpu.VMEM(observed.shape, f32),
            pltpu.VMEM(obs_var.shape, f32),
            pltpu.SMEM(ridge.shape, f32),
            pltpu.SMEM(pred_back.shape, jnp.int32),
            pltpu.SemaphoreType.DMA((6,)),
            pltpu.VMEM((nb, 2 * SUB, members), f32),
            by_block,
            by_block,
            pltpu.SemaphoreType.DMA((1 + 2 * PARTS,)),
            pltpu.SemaphoreType.DMA((1 + 2 * PARTS,)),
            pltpu.VMEM((REACH + 1, SUB, LANES), f32),
            pltpu.VMEM((HALF // 2, 2 * nb, 2 * LANES), jnp.bfloat16),
        ],
        compiler_params=pltpu.CompilerParams(
            collective_id=0, has_side_effects=True, vmem_limit_bytes=VMEM_GRANT
        ),
        name="whole",
    )(*[
        pltpu.with_memory_space_constraint(x, pltpu.HBM)
        for x in (bounds, ensemble, observed, obs_var, ridge, pred_back)
    ])
    return ensemble + z


def choose(n, ensemble, *rest):
    local, rows, members = ensemble.shape
    even = lax.axis_size("blk") % PLANES == 0 and local == 2
    if even and rows == n * SUB and members == LANES and 2 * n * local == LANES:
        return by_rows(n, ensemble, *rest)
    return on_device(ensemble, *rest)


def solution(mesh):
    return jax.shard_map(
        functools.partial(choose, mesh.size),
        mesh=mesh,
        in_specs=(
            P(("region", "blk"), None, None),
            P(("region", "blk"), None, None),
            P(("region", "blk"), None),
            P(("region", "blk")),
            P(("region", "blk"), None),
            P(),
        ),
        out_specs=P(("region", "blk"), None, None),
        check_vma=False,
    )
```
